32 devices in a mesh: dp: 2 (over x), fsdp: 4 (over z), ep: 4 (over y, core).
Axes of the slice: x: 2, y: 2, z: 4, core: 2. Of those that a mesh axis runs over, the one named last changes fastest.
Arguments:
- hidden: bfloat16 [65536, 4096], P(('dp', 'fsdp', 'ep')), parts along dimension 0
- norm_gain: bfloat16 [4096], replicated
- w_router: bfloat16 [4096, 16], replicated
- w_gate: bfloat16 [16, 4096, 688], P('ep', 'fsdp')
- w_up: bfloat16 [16, 4096, 688], P('ep', 'fsdp')
- w_down: bfloat16 [16, 688, 4096], P('ep', None, 'fsdp')
- top2_ids: int32 [65536, 2], P(('dp', 'fsdp', 'ep')), parts along dimension 0
Outputs:
- output: bfloat16 [65536, 4096], P(('dp', 'fsdp', 'ep')), parts along dimension 0
There are 2 independent parts. The reference program is written for one: setup_inputs(seed, part) draws one part's arguments, and reference() takes and returns one part's arrays. A program takes and returns all parts, laid end to end along the dimension named above; an argument that names none is the same for every part.
All inputs are finite; a program needn't handle non-finite values.
Results may differ from the reference program's by a relative error of at most 0.001.
Values are sent between devices in bfloat16 or wider.
A program may use at most 1 GiB of HBM per device.

```python
import jax
import jax.numpy as jnp
import numpy as np
from jax import lax

D = 4096
FF = 688
EXPERTS = 16
TOKENS_DEV = 2048
GROUPS = 16
TOKENS = GROUPS * TOKENS_DEV
CAPACITY = (5 * TOKENS_DEV + 2 * EXPERTS - 1) // (2 * EXPERTS)
EPS = 1e-5


def draw_routes(route_key):
    perm_key, first_key, second_key = jax.random.split(route_key, 3)
    hot_count = max(EXPERTS // 4, 1)
    route_table = jnp.asarray(np.repeat(np.arange(EXPERTS), np.where(np.arange(EXPERTS) < hot_count, 4, 1)), dtype=jnp.int32)
    expert_perm = jax.random.permutation(perm_key, EXPERTS)
    table_pick = jax.random.randint(first_key, (TOKENS,), 0, route_table.shape[0])
    local_index = jnp.arange(TOKENS, dtype=jnp.int32) % TOKENS_DEV
    first_choice = jnp.where(local_index < EXPERTS, local_index, expert_perm[route_table[table_pick]])
    second_shift = jax.random.randint(second_key, (TOKENS,), 1, EXPERTS)
    second_choice = (first_choice + second_shift) % EXPERTS
    return jnp.stack([first_choice, second_choice], axis=1).astype(jnp.int32)


def setup_inputs(seed: int = 0, part: int = 0) -> dict:
    part_key = jax.random.fold_in(jax.random.key(seed), part)
    hidden_key, route_key = jax.random.split(part_key, 2)
    gain_key, router_key, gate_key, up_key, down_key = jax.random.split(jax.random.key(seed + 1), 5)
    hidden = jax.random.normal(hidden_key, (TOKENS, D), jnp.float32)
    norm_gain = jax.random.uniform(gain_key, (D,), jnp.float32, 0.5, 1.5)
    w_router = jax.random.normal(router_key, (D, EXPERTS), jnp.float32) * (0.5 * D ** -0.5)
    w_gate = jax.random.normal(gate_key, (EXPERTS, D, FF), jnp.float32) * D ** -0.5
    w_up = jax.random.normal(up_key, (EXPERTS, D, FF), jnp.float32) * D ** -0.5
    w_down = jax.random.normal(down_key, (EXPERTS, FF, D), jnp.float32) * FF ** -0.5
    return {
        'hidden': hidden.astype(jnp.bfloat16),
        'norm_gain': norm_gain.astype(jnp.bfloat16),
        'w_router': w_router.astype(jnp.bfloat16),
        'w_gate': w_gate.astype(jnp.bfloat16),
        'w_up': w_up.astype(jnp.bfloat16),
        'w_down': w_down.astype(jnp.bfloat16),
        'top2_ids': draw_routes(route_key),
    }


def expert_ffn(expert_pack):
    rows_in, gate_mat, up_mat, down_mat = expert_pack
    act_a = jnp.dot(rows_in, gate_mat, preferred_element_type=jnp.float32)
    act_b = jnp.dot(rows_in, up_mat, preferred_element_type=jnp.float32)
    hidden_act = (jax.nn.silu(act_a) * act_b).astype(jnp.bfloat16)
    return jnp.dot(hidden_act, down_mat, preferred_element_type=jnp.float32).astype(jnp.bfloat16)


def reference(hidden, norm_gain, w_router, w_gate, w_up, w_down, top2_ids):
    hidden_f32 = hidden.astype(jnp.float32)
    mean_sq = jnp.mean(hidden_f32 * hidden_f32, axis=-1, keepdims=True)
    normed = (hidden_f32 * lax.rsqrt(mean_sq + EPS) * norm_gain.astype(jnp.float32)).astype(jnp.bfloat16)
    logits = jnp.dot(normed, w_router, preferred_element_type=jnp.float32)
    gate_probs = jax.nn.softmax(jnp.take_along_axis(logits, top2_ids, axis=1), axis=-1)
    flat_ids = top2_ids.reshape(GROUPS, 2 * TOKENS_DEV)
    onehot = (flat_ids[:, :, None] == jnp.arange(EXPERTS, dtype=jnp.int32)).astype(jnp.int32)
    position = jnp.sum((jnp.cumsum(onehot, axis=1) - 1) * onehot, axis=2)
    group_base = jnp.arange(GROUPS, dtype=jnp.int32)[:, None] * (EXPERTS * CAPACITY)
    all_slots = GROUPS * EXPERTS * CAPACITY
    slot_ids = jnp.where(position < CAPACITY, group_base + flat_ids * CAPACITY + position, all_slots).reshape(TOKENS, 2)
    token_index = jnp.broadcast_to(jnp.arange(TOKENS, dtype=jnp.int32)[:, None], (TOKENS, 2))
    source = jnp.full((all_slots,), TOKENS, dtype=jnp.int32).at[slot_ids.reshape(-1)].set(token_index.reshape(-1), mode='drop')
    buffers = jnp.take(normed, source, axis=0, mode='fill', fill_value=0)
    by_expert = buffers.reshape(GROUPS, EXPERTS, CAPACITY, D).transpose(1, 0, 2, 3).reshape(EXPERTS, GROUPS * CAPACITY, D)
    expert_out = lax.map(expert_ffn, (by_expert, w_gate, w_up, w_down))
    out_flat = expert_out.reshape(EXPERTS, GROUPS, CAPACITY, D).transpose(1, 0, 2, 3).reshape(all_slots, D)
    returned = jnp.take(out_flat, slot_ids, axis=0, mode='fill', fill_value=0)
    moe_sum = jnp.sum(gate_probs[:, :, None] * returned.astype(jnp.float32), axis=1)
    return (hidden_f32 + moe_sum).astype(jnp.bfloat16)
```

```python
import functools

import jax
import jax.numpy as jnp
from jax import lax
from jax.experimental import pallas as pl
from jax.experimental.pallas import tpu as pltpu
from jax.sharding import PartitionSpec as P

EPS = 1e-5
MESH = pl.DeviceIdType.MESH
HBM = pl.BlockSpec(memory_space=pl.ANY)
VMEM = pl.BlockSpec(memory_space=pltpu.VMEM)
F = 4
E = 4
CHUNKS = 8


def exchange_kernel(hid, *refs):
    (wg, wu, wd, hall, gf, uf, df, own_sem, hy_s, hy_r, hs_s, hs_r, hf_s, hf_r,
     zr_s, zl_s, z_r, x_s, x_r) = refs
    half, z, j = lax.axis_index('dp'), lax.axis_index('fsdp'), lax.axis_index('ep')
    sib = j + 1 - 2 * (j % 2)
    across = (j + 2) % E
    experts, _, width = wg.shape
    part = width // 2
    rows = hid.shape[0] // CHUNKS
    pieces = [(src, dst, e) for e in range(experts) for src, dst in ((wg, gf), (wu, uf), (wd, df))]

    def region(p, f, h):
        return pieces[p][1].at[pieces[p][2], :, pl.ds(pl.multiple_of(f * width + h * part, 128), part)]

    def own(p):
        return pieces[p][0].at[pieces[p][2], :, pl.ds(pl.multiple_of(half * part, 128), part)]

    def along_z(p, f, src, step, sems):
        return pltpu.make_async_remote_copy(
            src_ref=src, dst_ref=region(p, f, half), send_sem=sems.at[p, f], recv_sem=z_r.at[p, f],
            device_id={'fsdp': z + step}, device_id_type=MESH)

    def along_x(p, f, h):
        return pltpu.make_async_remote_copy(
            src_ref=region(p, f, h), dst_ref=region(p, f, h), send_sem=x_s.at[p, f], recv_sem=x_r.at[p, f],
            device_id={'dp': 1 - half}, device_id_type=MESH)

    def tokens(src, owner, c, send, recv, target):
        return pltpu.make_async_remote_copy(
            src_ref=src, dst_ref=hall.at[owner, pl.ds(c * rows, rows)], send_sem=send.at[c], recv_sem=recv.at[c],
            device_id={'ep': target}, device_id_type=MESH)

    def mine(c):
        return hid.at[pl.ds(c * rows, rows)]

    def local(c):
        return pltpu.make_async_copy(mine(c), hall.at[j, pl.ds(c * rows, rows)], own_sem.at[c])

    for p in range(len(pieces)):
        pl.when(z < F - 1)(lambda p=p: along_z(p, z, own(p), 1, zr_s).start())
        pl.when(z > 0)(lambda p=p: along_z(p, z, own(p), -1, zl_s).start())
    for c in range(CHUNKS):
        tokens(mine(c), j, c, hy_s, hy_r, across).start()
    for c in range(CHUNKS):
        tokens(mine(c), j, c, hs_s, hs_r, sib).start()
        local(c).start()

    def arrive(p, d):
        def from_left():
            f = z - d
            along_z(p, f, own(p), 1, zr_s).wait_recv()
            pl.when(z < F - 1)(lambda: along_z(p, f, region(p, f, half), 1, zr_s).start())
            along_x(p, f, half).start()

        def from_right():
            f = z + d
            along_z(p, f, own(p), 1, zr_s).wait_recv()
            pl.when(z > 0)(lambda: along_z(p, f, region(p, f, half), -1, zl_s).start())
            along_x(p, f, half).start()

        pl.when(z >= d)(from_left)
        pl.when(z < F - d)(from_right)

    total = (F - 1) * len(pieces)
    done = 0
    for i, (d, p) in enumerate((d, p) for d in range(1, F) for p in range(len(pieces))):
        arrive(p, d)
        while done < CHUNKS and (done + 1) * total * 3 <= (i + 1) * CHUNKS * 4:
            tokens(mine(done), across, done, hy_s, hy_r, across).wait_recv()
            tokens(hall.at[across, pl.ds(done * rows, rows)], across, done, hf_s, hf_r, sib).start()
            done += 1
    for c in range(CHUNKS):
        tokens(mine(c), j, c, hy_s, hy_r, across).wait_send()
        tokens(mine(c), j, c, hs_s, hs_r, sib).wait()
        tokens(mine(c), j, c, hf_s, hf_r, sib).wait()
        local(c).wait()
    for p in range(len(pieces)):
        for f in range(F):
            def to_right(p=p, f=f):
                along_z(p, f, own(p), 1, zr_s).wait_send()

            def to_left(p=p, f=f):
                along_z(p, f, own(p), -1, zl_s).wait_send()

            def both(p=p, f=f):
                along_x(p, f, half).wait_send()
                along_x(p, f, 1 - half).wait_recv()

            pl.when(jnp.logical_and(z < F - 1, f <= z))(to_right)
            pl.when(jnp.logical_and(z > 0, f >= z))(to_left)
            pl.when(z != f)(both)


def exchange(hidden, w_gate, w_up, w_down):
    experts, ff, width = w_gate.shape
    full = jax.ShapeDtypeStruct((experts, ff, F * width), w_gate.dtype)
    dma = pltpu.SemaphoreType.DMA
    grid_sems = [dma((3 * experts, F)) for _ in range(5)]
    return pl.pallas_call(
        exchange_kernel,
        out_shape=(jax.ShapeDtypeStruct((E,) + hidden.shape, hidden.dtype), full, full, full),
        in_specs=[HBM] * 4,
        out_specs=(HBM,) * 4,
        scratch_shapes=[dma((CHUNKS,)) for _ in range(7)] + grid_sems,
        compiler_params=pltpu.CompilerParams(has_side_effects=True),
        name='exchange',
    )(hidden, w_gate, w_up, w_down)


O_SLOTS = 4


def expert_kernel(rows_in, gain, wg, wu, wd, gf, uf, df, back, wbuf, xbuf, obuf, hbuf, acc_a, acc_b,
                  w_sem, x_sem, o_sem, r_sem):
    z, j = lax.axis_index('fsdp'), lax.axis_index('ep')
    y, core = j // 2, j % 2
    experts, _, capacity, d_model = rows_in.shape
    width = wg.shape[2]
    blocks = experts * E
    sources = ((wg, gf), (wu, uf), (wd, df))

    def owner(q):
        return ((y + 1 - q // 2) % 2) * 2 + (core + q % 2) % 2

    def weights(e, act):
        slot = e % 2
        for t, (part, whole) in enumerate(sources):
            for f in range(F):
                cols = pl.ds(f * width, width)
                dst, sem = wbuf.at[slot, t, :, cols], w_sem.at[slot, t * F + f]
                pl.when(z == f)(lambda: act(pltpu.make_async_copy(part.at[e], dst, sem)))
                pl.when(z != f)(lambda: act(pltpu.make_async_copy(whole.at[e, :, cols], dst, sem)))

    def x_load(i):
        return pltpu.make_async_copy(rows_in.at[i // E, owner(i % E)], xbuf.at[i % 2], x_sem.at[i % 2])

    def send(i):
        return pltpu.make_async_remote_copy(
            src_ref=obuf.at[i % O_SLOTS], dst_ref=back.at[j * experts + i // E], send_sem=o_sem.at[i % O_SLOTS],
            recv_sem=r_sem.at[j * experts + i // E], device_id={'ep': owner(i % E)}, device_id_type=MESH)

    def keep(i):
        return pltpu.make_async_copy(obuf.at[i % O_SLOTS], back.at[j * experts + i // E], o_sem.at[i % O_SLOTS])

    def sent(i):
        pl.when(i % E == 2)(lambda: keep(i).wait())
        pl.when(i % E != 2)(lambda: send(i).wait_send())

    weights(0, lambda copy: copy.start())
    x_load(0).start()

    def block(i, carry):
        e = i // E
        slot, xs, os = e % 2, i % 2, i % O_SLOTS

        @pl.when(i % E == 0)
        def _():
            weights(e, lambda copy: copy.wait())
            pl.when(e + 1 < experts)(lambda: weights(e + 1, lambda copy: copy.start()))

        x_load(i).wait()
        pl.when(i + 1 < blocks)(lambda: x_load(i + 1).start())

        step = 16 if capacity % 16 == 0 else capacity
        def norm(r, c):
            rs = pl.ds(pl.multiple_of(r * step, step), step)
            x = xbuf[xs, rs, :].astype(jnp.float32)
            scale = lax.rsqrt(jnp.mean(x * x, axis=-1, keepdims=True) + EPS)
            xbuf[xs, rs, :] = (x * scale * gain[...]).astype(jnp.bfloat16)
            return c
        lax.fori_loop(0, capacity // step, norm, 0)

        acc_a[...] = jnp.zeros_like(acc_a)
        acc_b[...] = jnp.zeros_like(acc_b)
        def first(k, c):
            ks = pl.ds(pl.multiple_of(k * width, 128), width)
            u = xbuf[xs, :, ks]
            dims = (((1,), (1,)), ((), ()))
            acc_a[...] += lax.dot_general(u, wbuf[slot, 0, :, ks], dims, preferred_element_type=jnp.float32)
            acc_b[...] += lax.dot_general(u, wbuf[slot, 1, :, ks], dims, preferred_element_type=jnp.float32)
            return c
        lax.fori_loop(0, F, first, 0)
        a = acc_a[...]
        hbuf[...] = (a * jax.nn.sigmoid(a) * acc_b[...]).astype(jnp.bfloat16)

        pl.when(i >= O_SLOTS)(lambda: sent(i - O_SLOTS))
        def second(n, c):
            ns = pl.ds(pl.multiple_of(n * width, 128), width)
            obuf[os, :, ns] = jnp.dot(
                hbuf[...], wbuf[slot, 2, :, ns], preferred_element_type=jnp.float32).astype(jnp.bfloat16)
            return c
        lax.fori_loop(0, F, second, 0)
        pl.when(i % E == 2)(lambda: keep(i).start())
        pl.when(i % E != 2)(lambda: send(i).start())
        return carry

    lax.fori_loop(0, blocks, block, 0)
    for i in range(blocks - O_SLOTS, blocks):
        sent(i)

    def arrived(n, c):
        def wait():
            pltpu.make_async_remote_copy(
                src_ref=obuf.at[0], dst_ref=back.at[n], send_sem=o_sem.at[0], recv_sem=r_sem.at[n],
                device_id={'ep': n // experts}, device_id_type=MESH).wait_recv()
        pl.when(n // experts != j)(wait)
        return c
    lax.fori_loop(0, blocks, arrived, 0)


def run_experts(rows_in, gain, w_gate, w_up, w_down, gate_full, up_full, down_full):
    experts, _, capacity, d_model = rows_in.shape
    ff = w_gate.shape[1]
    dma = pltpu.SemaphoreType.DMA
    return pl.pallas_call(
        expert_kernel,
        out_shape=jax.ShapeDtypeStruct((E * experts, capacity, d_model), jnp.bfloat16),
        in_specs=[HBM, VMEM] + [HBM] * 6,
        out_specs=HBM,
        scratch_shapes=[
            pltpu.VMEM((2, 3, ff, d_model), jnp.bfloat16),
            pltpu.VMEM((2, capacity, d_model), jnp.bfloat16),
            pltpu.VMEM((O_SLOTS, capacity, d_model), jnp.bfloat16),
            pltpu.VMEM((capacity, ff), jnp.bfloat16),
            pltpu.VMEM((capacity, ff), jnp.float32),
            pltpu.VMEM((capacity, ff), jnp.float32),
            dma((2, 3 * F)), dma((2,)), dma((O_SLOTS,)), dma((E * experts,)),
        ],
        compiler_params=pltpu.CompilerParams(has_side_effects=True, vmem_limit_bytes=62 * 1024 * 1024),
        name='experts',
    )(rows_in, gain, w_gate, w_up, w_down, gate_full, up_full, down_full)


def gate_values(hidden_f32, norm_gain, w_router, top2_ids):
    mean_sq = jnp.mean(hidden_f32 * hidden_f32, axis=-1, keepdims=True)
    normed = (hidden_f32 * lax.rsqrt(mean_sq + EPS) * norm_gain.astype(jnp.float32)).astype(jnp.bfloat16)
    logits = jnp.dot(normed, w_router, preferred_element_type=jnp.float32)
    experts = jnp.arange(w_router.shape[1], dtype=jnp.int32)
    picked = [jnp.sum(jnp.where(top2_ids[:, k:k + 1] == experts, logits, 0.0), axis=1) for k in range(2)]
    return jax.nn.softmax(jnp.stack(picked, axis=1), axis=-1)


def local_block(hidden, norm_gain, w_router, w_gate, w_up, w_down, top2_ids):
    tok_local, d_model = hidden.shape
    num_experts = w_router.shape[1]
    capacity = (5 * tok_local + 2 * num_experts - 1) // (2 * num_experts)
    experts = num_experts // E
    gate_t, up_t = jnp.swapaxes(w_gate, 1, 2), jnp.swapaxes(w_up, 1, 2)

    flat_ids = top2_ids.reshape(-1)
    onehot = (flat_ids[:, None] == jnp.arange(num_experts, dtype=jnp.int32)[None, :]).astype(jnp.int32)
    position = jnp.sum((jnp.cumsum(onehot, axis=0) - 1) * onehot, axis=1)
    keep = (position < capacity).reshape(top2_ids.shape)
    slot_ids = jnp.where(position < capacity, flat_ids * capacity + position, num_experts * capacity)
    token_index = jnp.arange(2 * tok_local, dtype=jnp.int32) // 2
    source = jnp.zeros((num_experts * capacity,), jnp.int32).at[slot_ids].set(token_index, mode='drop')
    source = lax.all_to_all(source.reshape(E, experts * capacity), 'ep', 0, 0)
    source = source.reshape(E, experts, capacity) + (jnp.arange(E, dtype=jnp.int32) * tok_local)[:, None, None]
    source = jnp.swapaxes(source, 0, 1).reshape(-1)

    everyone, gate_full, up_full, down_full = exchange(hidden, gate_t, up_t, w_down)
    rows_in = jnp.take(everyone.reshape(E * tok_local, d_model), source, axis=0, mode='clip')
    rows_in = rows_in.reshape(experts, E, capacity, d_model)
    gain = norm_gain.astype(jnp.float32).reshape(1, d_model)
    back = run_experts(rows_in, gain, gate_t, up_t, w_down, gate_full, up_full, down_full)
    back = back.reshape(num_experts * capacity, d_model)

    hidden_f32 = hidden.astype(jnp.float32)
    gate_probs = gate_values(hidden_f32, norm_gain, w_router, top2_ids)
    slot_ids = slot_ids.reshape(top2_ids.shape)
    moe = [
        jnp.where(keep[:, k:k + 1],
                  gate_probs[:, k:k + 1] * jnp.take(back, slot_ids[:, k], axis=0, mode='clip').astype(jnp.float32), 0.0)
        for k in range(2)
    ]
    return (hidden_f32 + (moe[0] + moe[1])).astype(jnp.bfloat16)


def solution(mesh):
    tok_spec = P(('dp', 'fsdp', 'ep'), None)
    in_specs = (tok_spec, P(None), P(None, None), P('ep', 'fsdp', None), P('ep', 'fsdp', None), P('ep', None, 'fsdp'), tok_spec)
    return jax.shard_map(local_block, mesh=mesh, in_specs=in_specs, out_specs=tok_spec, check_vma=False)
```

```python
import functools

import jax
import jax.numpy as jnp
from jax import lax
from jax.experimental import pallas as pl
from jax.experimental.pallas import tpu as pltpu
from jax.sharding import PartitionSpec as P

EPS = 1e-5
MESH = pl.DeviceIdType.MESH
HBM = pl.BlockSpec(memory_space=pl.ANY)
VMEM = pl.BlockSpec(memory_space=pltpu.VMEM)
F = 4
E = 4
CHUNKS = 8


O_SLOTS = 4
COLS = 8


def moe_kernel(hid, pos, gain, wg, wu, wd, back, hall, full, rows,
               wbuf, xbuf, obuf, hbuf, acc_a, acc_b, pick, tok, out,
               hy_s, hy_r, hs_s, hs_r, hf_s, hf_r, zr_s, zl_s, z_r, x_s, x_r,
               w_sem, x_sem, o_sem, r_sem, t_sem, g_sem):
    half, z, j = lax.axis_index('dp'), lax.axis_index('fsdp'), lax.axis_index('ep')
    y, core = j // 2, j % 2
    sib = j + 1 - 2 * core
    across = (j + 2) % E
    experts, ff, width = wg.shape
    part = width // 2
    tokens, d_model = hid.shape
    capacity = hbuf.shape[0]
    pair = 2 * capacity
    chunk = tokens // CHUNKS
    cols = d_model // COLS
    local = (wg, wu, wd)
    group = 3 * experts // 2
    steps = (F - 1) * group
    blocks = experts * E

    def region(p, f, h):
        return full.at[p % 3, p // 3, :, pl.ds(pl.multiple_of(f * width + h * part, 128), part)]

    def own(p):
        return local[p % 3].at[p // 3, :, pl.ds(pl.multiple_of(half * part, 128), part)]

    def along_z(p, f, src, step, sems):
        return pltpu.make_async_remote_copy(
            src_ref=src, dst_ref=region(p, f, half), send_sem=sems.at[p, f], recv_sem=z_r.at[p, f],
            device_id={'fsdp': z + step}, device_id_type=MESH)

    def along_x(p, f, h):
        return pltpu.make_async_remote_copy(
            src_ref=region(p, f, h), dst_ref=region(p, f, h), send_sem=x_s.at[p, f], recv_sem=x_r.at[p, f],
            device_id={'dp': 1 - half}, device_id_type=MESH)

    def own_start(lo, hi):
        for p in range(lo, hi):
            pl.when(z < F - 1)(lambda p=p: along_z(p, z, own(p), 1, zr_s).start())
            pl.when(z > 0)(lambda p=p: along_z(p, z, own(p), -1, zl_s).start())

    def arrive(p, d):
        def from_left():
            f = z - d
            along_z(p, f, region(p, f, half), 1, zr_s).wait_recv()
            pl.when(z < F - 1)(lambda: along_z(p, f, region(p, f, half), 1, zr_s).start())
            along_x(p, f, half).start()

        def from_right():
            f = z + d
            along_z(p, f, region(p, f, half), 1, zr_s).wait_recv()
            pl.when(z > 0)(lambda: along_z(p, f, region(p, f, half), -1, zl_s).start())
            along_x(p, f, half).start()

        pl.when(z >= d)(from_left)
        pl.when(z < F - d)(from_right)

    def arrivals(base, lo, hi):
        def body(i, c):
            arrive(base + i % group, i // group + 1)
            return c
        lax.fori_loop(lo, hi, body, 0)

    def each_piece(lo, hi, act):
        def body(i, c):
            p, f = lo + i // F, i % F
            act(p, f)
            return c
        lax.fori_loop(0, (hi - lo) * F, body, 0)

    def swapped(lo, hi):
        each_piece(lo, hi, lambda p, f: pl.when(z != f)(lambda: along_x(p, f, 1 - half).wait_recv()))

    def token_copy(src, owner, c, send, recv, target):
        return pltpu.make_async_remote_copy(
            src_ref=src, dst_ref=hall.at[owner, pl.ds(c * chunk, chunk)], send_sem=send.at[c], recv_sem=recv.at[c],
            device_id={'ep': target}, device_id_type=MESH)

    def mine(c):
        return hid.at[pl.ds(c * chunk, chunk)]

    def forward(lo, hi):
        for c in range(lo, hi):
            token_copy(mine(c), across, c, hy_s, hy_r, across).wait_recv()
            token_copy(hall.at[across, pl.ds(c * chunk, chunk)], across, c, hf_s, hf_r, sib).start()

    def device(ybit, cbit):
        return (y + ybit) % 2 * 2 + (core + cbit) % 2

    def token_load(r, n):
        owner = device(r // 4, r % 2)
        ns = pl.ds(pl.multiple_of(n * cols, 128), cols)
        near = pltpu.make_async_copy(hid.at[:, ns], tok.at[n % 2], t_sem.at[n % 2])
        far = pltpu.make_async_copy(hall.at[owner, :, ns], tok.at[n % 2], t_sem.at[n % 2])
        return near, far, r // 4 + r % 2 == 0

    def token_start(r, n):
        near, far, is_near = token_load(r, n)
        pl.when(is_near)(lambda: near.start())
        pl.when(jnp.logical_not(is_near))(lambda: far.start())

    def row_store(r, n):
        ns = pl.ds(pl.multiple_of(n * cols, 128), cols)
        dst = rows.at[r // 4 * 2 + r % 2, pl.ds(pl.multiple_of(r // 2 % 2 * pair, 16), pair), ns]
        return pltpu.make_async_copy(out.at[n % 2], dst, g_sem.at[n % 2])

    def pick_rows(r):
        token_start(r, 0)
        owner = device(r // 4, r % 2)
        step = 32 if capacity % 32 == 0 else capacity

        def mark(i, c):
            e = i // (capacity // step)
            first = (i % (capacity // step)) * step
            want = pos[owner * experts + r // 2 % 2 * 2 + e]
            slot = first + lax.broadcasted_iota(jnp.int32, (step, tokens), 0)
            pick[pl.ds(pl.multiple_of(i * step, step), step), :] = jnp.where(slot == want, 1.0, 0.0).astype(jnp.bfloat16)
            return c
        lax.fori_loop(0, pair // step, mark, 0)

        def column(n, c):
            near, _, _ = token_load(r, n)
            near.wait()
            pl.when(n + 1 < COLS)(lambda: token_start(r, n + 1))
            pl.when(n >= 2)(lambda: row_store(r, n - 2).wait())
            out[n % 2] = jnp.dot(pick[...], tok[n % 2], preferred_element_type=jnp.float32).astype(jnp.bfloat16)
            row_store(r, n).start()
            return c
        lax.fori_loop(0, COLS, column, 0)
        row_store(r, COLS - 2).wait()
        row_store(r, COLS - 1).wait()

    def weights(e, act):
        slot = e % 2
        for t in range(3):
            for f in range(F):
                fs = pl.ds(f * width, width)
                dst, sem = wbuf.at[slot, t, :, fs], w_sem.at[slot, t * F + f]
                pl.when(z == f)(lambda: act(pltpu.make_async_copy(local[t].at[e], dst, sem)))
                pl.when(z != f)(lambda: act(pltpu.make_async_copy(full.at[t, e, :, fs], dst, sem)))

    def start(copy):
        copy.start()

    def wait(copy):
        copy.wait()

    def place(k):
        m = k - 8
        e = jnp.where(k < 4, k // 2, jnp.where(k < 8, k % 2, 2 + m // 4))
        ybit = jnp.where(k < 4, 0, jnp.where(k < 8, 1, 1 - m % 2))
        cbit = jnp.where(k < 4, k % 2, jnp.where(k < 8, (k - 4) // 2, m % 4 // 2))
        return e, ybit, cbit

    def x_load(k):
        e, ybit, cbit = place(k)
        src = rows.at[ybit * 2 + cbit, pl.ds(pl.multiple_of(e * capacity, 16), capacity)]
        return pltpu.make_async_copy(src, xbuf.at[k % 2], x_sem.at[k % 2])

    def send(k):
        e, ybit, cbit = place(k)
        return pltpu.make_async_remote_copy(
            src_ref=obuf.at[k % O_SLOTS], dst_ref=back.at[j * experts + e], send_sem=o_sem.at[k % O_SLOTS],
            recv_sem=r_sem.at[j * experts + e], device_id={'ep': device(ybit, cbit)}, device_id_type=MESH)

    def keep(k):
        e, _, _ = place(k)
        return pltpu.make_async_copy(obuf.at[k % O_SLOTS], back.at[j * experts + e], o_sem.at[k % O_SLOTS])

    def is_local(k):
        _, ybit, cbit = place(k)
        return ybit + cbit == 0

    def sent(k):
        pl.when(is_local(k))(lambda: keep(k).wait())
        pl.when(jnp.logical_not(is_local(k)))(lambda: send(k).wait_send())

    def block(k, last):
        e, _, _ = place(k)
        slot, xs, os = e % 2, k % 2, k % O_SLOTS
        pl.when(k < 4)(lambda: arrivals(group, k, k + 1))
        for at, lo, hi in ((4, 5, 8), (5, 8, 9), (6, 9, 11), (7, 11, 13)):
            pl.when(k == at)(lambda: arrivals(group, lo, hi))

        @pl.when(k == 8)
        def _():
            arrivals(group, 13, steps)
            swapped(group, 2 * group)
            weights(2, start)
            weights(3, start)
            weights(2, wait)
        pl.when(k == 0)(lambda: weights(0, wait))
        pl.when(k == 2)(lambda: weights(1, wait))
        pl.when(k == 12)(lambda: weights(3, wait))

        x_load(k).wait()
        pl.when(k + 1 < last)(lambda: x_load(k + 1).start())

        step = 16 if capacity % 16 == 0 else capacity
        def norm(r, c):
            rs = pl.ds(pl.multiple_of(r * step, step), step)
            x = xbuf[xs, rs, :].astype(jnp.float32)
            scale = lax.rsqrt(jnp.mean(x * x, axis=-1, keepdims=True) + EPS)
            xbuf[xs, rs, :] = (x * scale * gain[...]).astype(jnp.bfloat16)
            return c
        lax.fori_loop(0, capacity // step, norm, 0)

        acc_a[...] = jnp.zeros_like(acc_a)
        acc_b[...] = jnp.zeros_like(acc_b)
        def first(i, c):
            ks = pl.ds(pl.multiple_of(i * width, 128), width)
            u = xbuf[xs, :, ks]
            dims = (((1,), (1,)), ((), ()))
            acc_a[...] += lax.dot_general(u, wbuf[slot, 0, :, ks], dims, preferred_element_type=jnp.float32)
            acc_b[...] += lax.dot_general(u, wbuf[slot, 1, :, ks], dims, preferred_element_type=jnp.float32)
            return c
        lax.fori_loop(0, F, first, 0)
        a = acc_a[...]
        hbuf[...] = (a * jax.nn.sigmoid(a) * acc_b[...]).astype(jnp.bfloat16)

        pl.when(k >= O_SLOTS)(lambda: sent(k - O_SLOTS))
        def second(i, c):
            ns = pl.ds(pl.multiple_of(i * width, 128), width)
            obuf[os, :, ns] = jnp.dot(
                hbuf[...], wbuf[slot, 2, :, ns], preferred_element_type=jnp.float32).astype(jnp.bfloat16)
            return c
        lax.fori_loop(0, F, second, 0)
        pl.when(is_local(k))(lambda: keep(k).start())
        pl.when(jnp.logical_not(is_local(k)))(lambda: send(k).start())
        return last

    for c in range(CHUNKS):
        token_copy(mine(c), j, c, hs_s, hs_r, sib).start()
        token_copy(mine(c), j, c, hy_s, hy_r, across).start()
    own_start(0, group)

    def round_(r, c):
        @pl.when(r == 1)
        def _():
            for c in range(CHUNKS):
                token_copy(mine(c), sib, c, hs_s, hs_r, sib).wait_recv()

        @pl.when(r == 4)
        def _():
            forward(6, CHUNKS)
            arrivals(group, 4, 5)

        @pl.when(r == 5)
        def _():
            for c in range(CHUNKS):
                token_copy(mine(c), sib, c, hf_s, hf_r, sib).wait_recv()

        pick_rows(r)
        pl.when(r == 1)(lambda: arrivals(0, 0, 2))
        pl.when(r == 2)(lambda: arrivals(0, 2, 4))

        @pl.when(r == 3)
        def _():
            arrivals(0, 4, 6)
            forward(0, 2)
            arrivals(0, 6, 9)
            forward(2, 3)
            arrivals(0, 9, 12)
            forward(3, 4)
            own_start(group, 2 * group)
            arrivals(0, 12, 15)
            forward(4, 5)
            arrivals(0, 15, steps)
            forward(5, 6)
            swapped(0, group)
            weights(0, start)
            weights(1, start)

        def upto(r):
            return (jnp.where(r >= 3, 4, 0) + jnp.where(r >= 4, 2, 0) + jnp.where(r >= 5, 2, 0) + jnp.where(r >= 7, 8, 0))
        lo, hi = upto(r - 1), upto(r)
        pl.when(lo < hi)(lambda: x_load(lo).start())
        lax.fori_loop(lo, hi, lambda k, last: block(k, last), hi)
        return c

    lax.fori_loop(0, 8, round_, 0)

    for k in range(blocks - O_SLOTS, blocks):
        sent(jnp.int32(k))
    for c in range(CHUNKS):
        token_copy(mine(c), j, c, hy_s, hy_r, across).wait_send()
        token_copy(mine(c), j, c, hs_s, hs_r, sib).wait_send()
        token_copy(mine(c), j, c, hf_s, hf_r, sib).wait_send()

    def drain(p, f):
        src = region(p, f, half)
        pl.when(jnp.logical_and(z < F - 1, f <= z))(lambda: along_z(p, f, src, 1, zr_s).wait_send())
        pl.when(jnp.logical_and(z > 0, f >= z))(lambda: along_z(p, f, src, -1, zl_s).wait_send())
        pl.when(z != f)(lambda: along_x(p, f, half).wait_send())
    each_piece(0, 2 * group, drain)

    def arrived(n, c):
        def wait_block():
            pltpu.make_async_remote_copy(
                src_ref=obuf.at[0], dst_ref=back.at[n], send_sem=o_sem.at[0], recv_sem=r_sem.at[n],
                device_id={'ep': n // experts}, device_id_type=MESH).wait_recv()
        pl.when(n // experts != j)(wait_block)
        return c
    lax.fori_loop(0, blocks, arrived, 0)


def run_moe(hidden, positions, gain, w_gate, w_up, w_down, capacity):
    tokens, d_model = hidden.shape
    experts, ff, width = w_gate.shape
    bf16, f32, dma = jnp.bfloat16, jnp.float32, pltpu.SemaphoreType.DMA
    pieces = 3 * experts
    shapes = (
        (E * experts, capacity, d_model),
        (E, tokens, d_model),
        (3, experts, ff, d_model),
        (E, experts * capacity, d_model),
    )
    return pl.pallas_call(
        moe_kernel,
        out_shape=tuple(jax.ShapeDtypeStruct(shape, bf16) for shape in shapes),
        in_specs=[HBM, VMEM, VMEM] + [HBM] * 3,
        out_specs=(HBM,) * 4,
        scratch_shapes=[
            pltpu.VMEM((2, 3, ff, d_model), bf16),
            pltpu.VMEM((2, capacity, d_model), bf16),
            pltpu.VMEM((O_SLOTS, capacity, d_model), bf16),
            pltpu.VMEM((capacity, ff), bf16),
            pltpu.VMEM((capacity, ff), f32),
            pltpu.VMEM((capacity, ff), f32),
            pltpu.VMEM((2 * capacity, tokens), bf16),
            pltpu.VMEM((2, tokens, d_model // COLS), bf16),
            pltpu.VMEM((2, 2 * capacity, d_model // COLS), bf16),
        ] + [dma((CHUNKS,)) for _ in range(6)] + [dma((pieces, F)) for _ in range(5)] + [
            dma((2, 3 * F)), dma((2,)), dma((O_SLOTS,)), dma((E * experts,)), dma((2,)), dma((2,)),
        ],
        compiler_params=pltpu.CompilerParams(has_side_effects=True, vmem_limit_bytes=63 * 1024 * 1024),
        name='moe',
    )(hidden, positions, gain, w_gate, w_up, w_down)[0]


def gate_values(hidden_f32, norm_gain, w_router, top2_ids):
    mean_sq = jnp.mean(hidden_f32 * hidden_f32, axis=-1, keepdims=True)
    normed = (hidden_f32 * lax.rsqrt(mean_sq + EPS) * norm_gain.astype(jnp.float32)).astype(jnp.bfloat16)
    logits = jnp.dot(normed, w_router, preferred_element_type=jnp.float32)
    experts = jnp.arange(w_router.shape[1], dtype=jnp.int32)
    picked = [jnp.sum(jnp.where(top2_ids[:, k:k + 1] == experts, logits, 0.0), axis=1) for k in range(2)]
    return jax.nn.softmax(jnp.stack(picked, axis=1), axis=-1)


def local_block(hidden, norm_gain, w_router, w_gate, w_up, w_down, top2_ids):
    tok_local, d_model = hidden.shape
    num_experts = w_router.shape[1]
    capacity = (5 * tok_local + 2 * num_experts - 1) // (2 * num_experts)
    experts = num_experts // E

    ids = [top2_ids[:, k][None, :] for k in range(2)]
    expert_ids = jnp.arange(num_experts, dtype=jnp.int32)[:, None]
    chosen = jnp.logical_or(ids[0] == expert_ids, ids[1] == expert_ids)
    before = jnp.cumsum(chosen.astype(jnp.int32), axis=1) - 1
    positions = jnp.where(chosen, before, -1)
    place = [jnp.sum(jnp.where(ids[k] == expert_ids, before, 0), axis=0) for k in range(2)]
    positions = lax.all_to_all(positions.reshape(E, experts, tok_local), 'ep', 0, 0)
    positions = positions.reshape(E * experts, 1, tok_local)

    gain = norm_gain.astype(jnp.float32).reshape(1, d_model)
    back = run_moe(hidden, positions, gain, jnp.swapaxes(w_gate, 1, 2), jnp.swapaxes(w_up, 1, 2), w_down, capacity)
    back = back.reshape(num_experts * capacity, d_model)

    hidden_f32 = hidden.astype(jnp.float32)
    gate_probs = gate_values(hidden_f32, norm_gain, w_router, top2_ids)
    moe = []
    for k in range(2):
        returned = jnp.take(back, top2_ids[:, k] * capacity + place[k], axis=0, mode='clip').astype(jnp.float32)
        moe.append(jnp.where((place[k] < capacity)[:, None], gate_probs[:, k:k + 1] * returned, 0.0))
    return (hidden_f32 + (moe[0] + moe[1])).astype(jnp.bfloat16)


def solution(mesh):
    tok_spec = P(('dp', 'fsdp', 'ep'), None)
    in_specs = (tok_spec, P(None), P(None, None), P('ep', 'fsdp', None), P('ep', 'fsdp', None), P('ep', None, 'fsdp'), tok_spec)
    return jax.shard_map(local_block, mesh=mesh, in_specs=in_specs, out_specs=tok_spec, check_vma=False)
```

```python
import functools

import jax
import jax.numpy as jnp
from jax import lax
from jax.experimental import pallas as pl
from jax.experimental.pallas import tpu as pltpu
from jax.sharding import PartitionSpec as P

EPS = 1e-5
MESH = pl.DeviceIdType.MESH
HBM = pl.BlockSpec(memory_space=pl.ANY)
VMEM = pl.BlockSpec(memory_space=pltpu.VMEM)
F = 4
E = 4
CHUNKS = 8


O_SLOTS = 4
COLS = 8


def moe_kernel(hid, pos, gain, wg, wu, wd, back, hall, full, rows,
               wbuf, xbuf, obuf, hbuf, acc_a, acc_b, pick, tok, out,
               hy_s, hy_r, hs_s, hs_r, hf_s, hf_r, zr_s, zl_s, z_r, x_s, x_r,
               w_sem, x_sem, o_sem, r_sem, t_sem, g_sem):
    half, z, j = lax.axis_index('dp'), lax.axis_index('fsdp'), lax.axis_index('ep')
    y, core = j // 2, j % 2
    sib = j + 1 - 2 * core
    across = (j + 2) % E
    experts, ff, width = wg.shape
    part = width // 2
    tokens, d_model = hid.shape
    capacity = hbuf.shape[0]
    pair = 2 * capacity
    chunk = tokens // CHUNKS
    cols = d_model // COLS
    local = (wg, wu, wd)
    group = 3 * experts // 2
    steps = (F - 1) * group
    blocks = experts * E

    def region(p, f, h):
        return full.at[p % 3, p // 3, :, pl.ds(pl.multiple_of(f * width + h * part, 128), part)]

    def own(p):
        return local[p % 3].at[p // 3, :, pl.ds(pl.multiple_of(half * part, 128), part)]

    def along_z(p, f, src, step, sems):
        return pltpu.make_async_remote_copy(
            src_ref=src, dst_ref=region(p, f, half), send_sem=sems.at[p, f], recv_sem=z_r.at[p, f],
            device_id={'fsdp': z + step}, device_id_type=MESH)

    def along_x(p, f, h):
        return pltpu.make_async_remote_copy(
            src_ref=region(p, f, h), dst_ref=region(p, f, h), send_sem=x_s.at[p, f], recv_sem=x_r.at[p, f],
            device_id={'dp': 1 - half}, device_id_type=MESH)

    def own_start(lo, hi):
        for p in range(lo, hi):
            pl.when(z < F - 1)(lambda p=p: along_z(p, z, own(p), 1, zr_s).start())
            pl.when(z > 0)(lambda p=p: along_z(p, z, own(p), -1, zl_s).start())

    def arrive(p, d):
        def from_left():
            f = z - d
            along_z(p, f, region(p, f, half), 1, zr_s).wait_recv()
            pl.when(z < F - 1)(lambda: along_z(p, f, region(p, f, half), 1, zr_s).start())
            along_x(p, f, half).start()

        def from_right():
            f = z + d
            along_z(p, f, region(p, f, half), 1, zr_s).wait_recv()
            pl.when(z > 0)(lambda: along_z(p, f, region(p, f, half), -1, zl_s).start())
            along_x(p, f, half).start()

        pl.when(z >= d)(from_left)
        pl.when(z < F - d)(from_right)

    def arrivals(base, lo, hi):
        def body(i, c):
            arrive(base + i % group, i // group + 1)
            return c
        lax.fori_loop(lo, hi, body, 0)

    def each_piece(lo, hi, act):
        def body(i, c):
            p, f = lo + i // F, i % F
            act(p, f)
            return c
        lax.fori_loop(0, (hi - lo) * F, body, 0)

    def swapped(lo, hi):
        each_piece(lo, hi, lambda p, f: pl.when(z != f)(lambda: along_x(p, f, 1 - half).wait_recv()))

    def token_copy(src, owner, c, send, recv, target):
        return pltpu.make_async_remote_copy(
            src_ref=src, dst_ref=hall.at[owner, pl.ds(c * chunk, chunk)], send_sem=send.at[c], recv_sem=recv.at[c],
            device_id={'ep': target}, device_id_type=MESH)

    def mine(c):
        return hid.at[pl.ds(c * chunk, chunk)]

    def forward(lo, hi):
        for c in range(lo, hi):
            token_copy(mine(c), across, c, hy_s, hy_r, across).wait_recv()
            token_copy(hall.at[across, pl.ds(c * chunk, chunk)], across, c, hf_s, hf_r, sib).start()

    def device(ybit, cbit):
        return (y + ybit) % 2 * 2 + (core + cbit) % 2

    def token_load(r, n):
        owner = device(r // 4, r % 2)
        ns = pl.ds(pl.multiple_of(n * cols, 128), cols)
        near = pltpu.make_async_copy(hid.at[:, ns], tok.at[n % 2], t_sem.at[n % 2])
        far = pltpu.make_async_copy(hall.at[owner, :, ns], tok.at[n % 2], t_sem.at[n % 2])
        return near, far, r // 4 + r % 2 == 0

    def token_start(r, n):
        near, far, is_near = token_load(r, n)
        pl.when(is_near)(lambda: near.start())
        pl.when(jnp.logical_not(is_near))(lambda: far.start())

    def row_store(r, n):
        ns = pl.ds(pl.multiple_of(n * cols, 128), cols)
        dst = rows.at[r // 4 * 2 + r % 2, pl.ds(pl.multiple_of(r // 2 % 2 * pair, 16), pair), ns]
        return pltpu.make_async_copy(out.at[n % 2], dst, g_sem.at[n % 2])

    def pick_rows(r):
        token_start(r, 0)
        owner = device(r // 4, r % 2)
        step = 32 if capacity % 32 == 0 else capacity

        def mark(i, c):
            e = i // (capacity // step)
            first = (i % (capacity // step)) * step
            want = pos[owner * experts + r // 2 % 2 * 2 + e]
            slot = first + lax.broadcasted_iota(jnp.int32, (step, tokens), 0)
            pick[pl.ds(pl.multiple_of(i * step, step), step), :] = jnp.where(slot == want, 1.0, 0.0).astype(jnp.bfloat16)
            return c
        lax.fori_loop(0, pair // step, mark, 0)

        def column(n, c):
            near, _, _ = token_load(r, n)
            near.wait()
            pl.when(n + 1 < COLS)(lambda: token_start(r, n + 1))
            pl.when(n >= 2)(lambda: row_store(r, n - 2).wait())
            out[n % 2] = jnp.dot(pick[...], tok[n % 2], preferred_element_type=jnp.float32).astype(jnp.bfloat16)
            row_store(r, n).start()
            return c
        lax.fori_loop(0, COLS, column, 0)
        row_store(r, COLS - 2).wait()
        row_store(r, COLS - 1).wait()

    def weights(e, act):
        slot = e % 2
        for t in range(3):
            for f in range(F):
                fs = pl.ds(f * width, width)
                dst, sem = wbuf.at[slot, t, :, fs], w_sem.at[slot, t * F + f]
                pl.when(z == f)(lambda: act(pltpu.make_async_copy(local[t].at[e], dst, sem)))
                pl.when(z != f)(lambda: act(pltpu.make_async_copy(full.at[t, e, :, fs], dst, sem)))

    def start(copy):
        copy.start()

    def wait(copy):
        copy.wait()

    def place(k):
        m = k - 8
        e = jnp.where(k < 4, k // 2, jnp.where(k < 8, k % 2, 2 + m // 4))
        ybit = jnp.where(k < 4, 0, jnp.where(k < 8, 1, 1 - m % 2))
        cbit = jnp.where(k < 4, k % 2, jnp.where(k < 8, (k - 4) // 2, m % 4 // 2))
        return e, ybit, cbit

    def x_load(k):
        e, ybit, cbit = place(k)
        src = rows.at[ybit * 2 + cbit, pl.ds(pl.multiple_of(e * capacity, 16), capacity)]
        return pltpu.make_async_copy(src, xbuf.at[k % 2], x_sem.at[k % 2])

    def send(k):
        e, ybit, cbit = place(k)
        return pltpu.make_async_remote_copy(
            src_ref=obuf.at[k % O_SLOTS], dst_ref=back.at[j * experts + e], send_sem=o_sem.at[k % O_SLOTS],
            recv_sem=r_sem.at[j * experts + e], device_id={'ep': device(ybit, cbit)}, device_id_type=MESH)

    def keep(k):
        e, _, _ = place(k)
        return pltpu.make_async_copy(obuf.at[k % O_SLOTS], back.at[j * experts + e], o_sem.at[k % O_SLOTS])

    def is_local(k):
        _, ybit, cbit = place(k)
        return ybit + cbit == 0

    def sent(k):
        pl.when(is_local(k))(lambda: keep(k).wait())
        pl.when(jnp.logical_not(is_local(k)))(lambda: send(k).wait_send())

    def block(k, last):
        e, _, _ = place(k)
        slot, xs, os = e % 2, k % 2, k % O_SLOTS
        pl.when(k < 4)(lambda: arrivals(group, k, k + 1))
        for at, lo, hi in ((4, 5, 8), (5, 8, 9), (6, 9, 11), (7, 11, 13)):
            pl.when(k == at)(lambda: arrivals(group, lo, hi))

        @pl.when(k == 8)
        def _():
            arrivals(group, 13, steps)
            swapped(group, 2 * group)
            weights(2, start)
            weights(3, start)
            weights(2, wait)
        pl.when(k == 0)(lambda: weights(0, wait))
        pl.when(k == 2)(lambda: weights(1, wait))
        pl.when(k == 12)(lambda: weights(3, wait))

        x_load(k).wait()
        pl.when(k + 1 < last)(lambda: x_load(k + 1).start())

        step = 16 if capacity % 16 == 0 else capacity
        def norm(r, c):
            rs = pl.ds(pl.multiple_of(r * step, step), step)
            x = xbuf[xs, rs, :].astype(jnp.float32)
            scale = lax.rsqrt(jnp.mean(x * x, axis=-1, keepdims=True) + EPS)
            xbuf[xs, rs, :] = (x * scale * gain[...]).astype(jnp.bfloat16)
            return c
        lax.fori_loop(0, capacity // step, norm, 0)

        acc_a[...] = jnp.zeros_like(acc_a)
        acc_b[...] = jnp.zeros_like(acc_b)
        def first(i, c):
            ks = pl.ds(pl.multiple_of(i * width, 128), width)
            u = xbuf[xs, :, ks]
            dims = (((1,), (1,)), ((), ()))
            acc_a[...] += lax.dot_general(u, wbuf[slot, 0, :, ks], dims, preferred_element_type=jnp.float32)
            acc_b[...] += lax.dot_general(u, wbuf[slot, 1, :, ks], dims, preferred_element_type=jnp.float32)
            return c
        lax.fori_loop(0, F, first, 0)
        a = acc_a[...]
        hbuf[...] = (a * jax.nn.sigmoid(a) * acc_b[...]).astype(jnp.bfloat16)

        pl.when(k >= O_SLOTS)(lambda: sent(k - O_SLOTS))
        def second(i, c):
            ns = pl.ds(pl.multiple_of(i * width, 128), width)
            obuf[os, :, ns] = jnp.dot(
                hbuf[...], wbuf[slot, 2, :, ns], preferred_element_type=jnp.float32).astype(jnp.bfloat16)
            return c
        lax.fori_loop(0, F, second, 0)
        pl.when(is_local(k))(lambda: keep(k).start())
        pl.when(jnp.logical_not(is_local(k)))(lambda: send(k).start())
        return last

    for c in range(CHUNKS):
        token_copy(mine(c), j, c, hs_s, hs_r, sib).start()
        token_copy(mine(c), j, c, hy_s, hy_r, across).start()
    own_start(0, group)

    def round_(r, c):
        @pl.when(r == 1)
        def _():
            for c in range(CHUNKS):
                token_copy(mine(c), sib, c, hs_s, hs_r, sib).wait_recv()

        @pl.when(r == 4)
        def _():
            forward(6, CHUNKS)
            arrivals(group, 4, 5)

        @pl.when(r == 5)
        def _():
            for c in range(CHUNKS):
                token_copy(mine(c), sib, c, hf_s, hf_r, sib).wait_recv()

        pick_rows(r)
        pl.when(r == 1)(lambda: arrivals(0, 0, 2))
        pl.when(r == 2)(lambda: arrivals(0, 2, 4))

        @pl.when(r == 3)
        def _():
            arrivals(0, 4, 6)
            forward(0, 2)
            arrivals(0, 6, 9)
            forward(2, 3)
            arrivals(0, 9, 12)
            forward(3, 4)
            own_start(group, 2 * group)
            arrivals(0, 12, 15)
            forward(4, 5)
            arrivals(0, 15, steps)
            forward(5, 6)
            swapped(0, group)
            weights(0, start)
            weights(1, start)

        def upto(r):
            return (jnp.where(r >= 3, 4, 0) + jnp.where(r >= 4, 2, 0) + jnp.where(r >= 5, 2, 0) + jnp.where(r >= 7, 8, 0))
        lo, hi = upto(r - 1), upto(r)
        pl.when(lo < hi)(lambda: x_load(lo).start())
        lax.fori_loop(lo, hi, lambda k, last: block(k, last), hi)
        return c

    lax.fori_loop(0, 8, round_, 0)

    for k in range(blocks - O_SLOTS, blocks):
        sent(jnp.int32(k))
    for c in range(CHUNKS):
        token_copy(mine(c), j, c, hy_s, hy_r, across).wait_send()
        token_copy(mine(c), j, c, hs_s, hs_r, sib).wait_send()
        token_copy(mine(c), j, c, hf_s, hf_r, sib).wait_send()

    def drain(p, f):
        src = region(p, f, half)
        pl.when(jnp.logical_and(z < F - 1, f <= z))(lambda: along_z(p, f, src, 1, zr_s).wait_send())
        pl.when(jnp.logical_and(z > 0, f >= z))(lambda: along_z(p, f, src, -1, zl_s).wait_send())
        pl.when(z != f)(lambda: along_x(p, f, half).wait_send())
    each_piece(0, 2 * group, drain)

    def arrived(n, c):
        def wait_block():
            pltpu.make_async_remote_copy(
                src_ref=obuf.at[0], dst_ref=back.at[n], send_sem=o_sem.at[0], recv_sem=r_sem.at[n],
                device_id={'ep': n // experts}, device_id_type=MESH).wait_recv()
        pl.when(n // experts != j)(wait_block)
        return c
    lax.fori_loop(0, blocks, arrived, 0)


def run_moe(hidden, positions, gain, w_gate, w_up, w_down, capacity):
    tokens, d_model = hidden.shape
    experts, ff, width = w_gate.shape
    bf16, f32, dma = jnp.bfloat16, jnp.float32, pltpu.SemaphoreType.DMA
    pieces = 3 * experts
    shapes = (
        (E * experts, capacity, d_model),
        (E, tokens, d_model),
        (3, experts, ff, d_model),
        (E, experts * capacity, d_model),
    )
    return pl.pallas_call(
        moe_kernel,
        out_shape=tuple(jax.ShapeDtypeStruct(shape, bf16) for shape in shapes),
        in_specs=[HBM, VMEM, VMEM] + [HBM] * 3,
        out_specs=(HBM,) * 4,
        scratch_shapes=[
            pltpu.VMEM((2, 3, ff, d_model), bf16),
            pltpu.VMEM((2, capacity, d_model), bf16),
            pltpu.VMEM((O_SLOTS, capacity, d_model), bf16),
            pltpu.VMEM((capacity, ff), bf16),
            pltpu.VMEM((capacity, ff), f32),
            pltpu.VMEM((capacity, ff), f32),
            pltpu.VMEM((2 * capacity, tokens), bf16),
            pltpu.VMEM((2, tokens, d_model // COLS), bf16),
            pltpu.VMEM((2, 2 * capacity, d_model // COLS), bf16),
        ] + [dma((CHUNKS,)) for _ in range(6)] + [dma((pieces, F)) for _ in range(5)] + [
            dma((2, 3 * F)), dma((2,)), dma((O_SLOTS,)), dma((E * experts,)), dma((2,)), dma((2,)),
        ],
        compiler_params=pltpu.CompilerParams(has_side_effects=True, vmem_limit_bytes=63 * 1024 * 1024),
        name='moe',
    )(hidden, positions, gain, w_gate, w_up, w_down)[0]


TILE = 128
SPAN = 16
WINDOWS = 32


def combine_kernel(starts, slots, probs, hid, back, out, buf, base, count, acc, sem):
    i = pl.program_id(0)
    num_experts = starts.shape[0] // (pl.num_programs(0) + 1)
    capacity = back.shape[0] // num_experts
    d_model = back.shape[1]
    cols = d_model // 4

    def window(row, s, n):
        src = back.at[pl.ds(pl.multiple_of(row, SPAN), SPAN)]
        return pltpu.make_async_copy(src, buf.at[s, pl.ds(pl.multiple_of(n * SPAN, SPAN), SPAN)], sem.at[s])

    def fill(tile, turn, s):
        first = turn * WINDOWS

        def clear(n, c):
            base[s, n] = -100000
            return c
        lax.fori_loop(0, WINDOWS, clear, 0)

        def expert(e, n):
            lo, hi = starts[tile * num_experts + e], starts[(tile + 1) * num_experts + e]

            def one(c, n):
                @pl.when(jnp.logical_and(n >= first, n < first + WINDOWS))
                def _():
                    row = e * capacity + c * SPAN
                    base[s, n - first] = row
                    window(row, s, n - first).start()
                return n + 1
            return lax.fori_loop(lo // SPAN, jnp.where(hi > lo, (hi + SPAN - 1) // SPAN, lo // SPAN), one, n)
        count[s] = lax.fori_loop(0, num_experts, expert, jnp.int32(0))

    def use(turn, s):
        def arrived(n, c):
            window(0, s, 0).wait()
            return c
        lax.fori_loop(0, jnp.minimum(count[s] - turn * WINDOWS, WINDOWS), arrived, 0)
        lane = lax.broadcasted_iota(jnp.int32, (1, WINDOWS * SPAN), 1)
        row = jnp.zeros_like(lane)
        for n in range(WINDOWS):
            row = jnp.where(lane // SPAN == n, base[s, n], row)
        row = row + lane % SPAN
        pick = jnp.where(slots[0] == row, 1.0, 0.0).astype(jnp.bfloat16)
        p0, p1 = probs[0, :TILE], probs[0, TILE:]

        def column(n, c):
            ns = pl.ds(pl.multiple_of(n * cols, 128), cols)
            got = jnp.dot(pick, buf[s, :, ns], preferred_element_type=jnp.float32)
            acc[:, ns] += p0 * got[:TILE] + p1 * got[TILE:]
            return c
        lax.fori_loop(0, 4, column, 0)

    s = i % 2

    @pl.when(i == 0)
    def _():
        buf[...] = jnp.zeros_like(buf)
        fill(i, 0, s)
    pl.when(i + 1 < pl.num_programs(0))(lambda: fill(i + 1, 0, 1 - s))
    acc[...] = hid[...].astype(jnp.float32)
    use(0, s)

    def more(turn, c):
        fill(i, turn, s)
        use(turn, s)
        return c
    lax.fori_loop(1, (count[s] + WINDOWS - 1) // WINDOWS, more, 0)
    out[...] = acc[...].astype(out.dtype)


def combine(hidden, back, starts, slots, probs):
    tokens, d_model = hidden.shape
    tiles = tokens // TILE
    column = pl.BlockSpec((1, 2 * TILE, 1), lambda i: (i, 0, 0))
    row = pl.BlockSpec((TILE, d_model), lambda i: (i, 0))

    def by_tile(x):
        return jnp.swapaxes(x.reshape(2, tiles, TILE), 0, 1).reshape(tiles, 2 * TILE, 1)
    return pl.pallas_call(
        combine_kernel,
        grid=(tiles,),
        out_shape=jax.ShapeDtypeStruct(hidden.shape, hidden.dtype),
        in_specs=[pl.BlockSpec(memory_space=pltpu.SMEM), column, column, row, HBM],
        out_specs=row,
        scratch_shapes=[
            pltpu.VMEM((2, WINDOWS * SPAN, d_model), jnp.bfloat16),
            pltpu.SMEM((2, WINDOWS), jnp.int32),
            pltpu.SMEM((2,), jnp.int32),
            pltpu.VMEM((TILE, d_model), jnp.float32),
            pltpu.SemaphoreType.DMA((2,)),
        ],
        compiler_params=pltpu.CompilerParams(dimension_semantics=('arbitrary',)),
        name='combine',
    )(starts.reshape(-1), by_tile(slots), by_tile(probs), hidden, back)


def gate_values(hidden_f32, norm_gain, w_router, top2_ids):
    mean_sq = jnp.mean(hidden_f32 * hidden_f32, axis=-1, keepdims=True)
    normed = (hidden_f32 * lax.rsqrt(mean_sq + EPS) * norm_gain.astype(jnp.float32)).astype(jnp.bfloat16)
    logits = jnp.dot(normed, w_router, preferred_element_type=jnp.float32)
    experts = jnp.arange(w_router.shape[1], dtype=jnp.int32)
    picked = [jnp.sum(jnp.where(top2_ids[:, k:k + 1] == experts, logits, 0.0), axis=1) for k in range(2)]
    return jax.nn.softmax(jnp.stack(picked, axis=1), axis=-1)


def local_block(hidden, norm_gain, w_router, w_gate, w_up, w_down, top2_ids):
    tok_local, d_model = hidden.shape
    num_experts = w_router.shape[1]
    capacity = (5 * tok_local + 2 * num_experts - 1) // (2 * num_experts)
    experts = num_experts // E

    ids = [top2_ids[:, k][None, :] for k in range(2)]
    expert_ids = jnp.arange(num_experts, dtype=jnp.int32)[:, None]
    chosen = jnp.logical_or(ids[0] == expert_ids, ids[1] == expert_ids)
    before = jnp.cumsum(chosen.astype(jnp.int32), axis=1) - 1
    positions = jnp.where(chosen, before, -1)
    place = [jnp.sum(jnp.where(ids[k] == expert_ids, before, 0), axis=0) for k in range(2)]
    positions = lax.all_to_all(positions.reshape(E, experts, tok_local), 'ep', 0, 0)
    positions = positions.reshape(E * experts, 1, tok_local)

    gain = norm_gain.astype(jnp.float32).reshape(1, d_model)
    back = run_moe(hidden, positions, gain, jnp.swapaxes(w_gate, 1, 2), jnp.swapaxes(w_up, 1, 2), w_down, capacity)
    back = back.reshape(num_experts * capacity, d_model)

    gate_probs = gate_values(hidden.astype(jnp.float32), norm_gain, w_router, top2_ids)
    slots = jnp.stack([jnp.where(place[k] < capacity, top2_ids[:, k] * capacity + place[k], -1) for k in range(2)])
    counts = jnp.minimum(before[:, TILE - 1::TILE].T + 1, capacity)
    starts = jnp.concatenate([jnp.zeros((1, num_experts), jnp.int32), counts], axis=0)
    return combine(hidden, back, starts, slots, gate_probs.T)


def solution(mesh):
    tok_spec = P(('dp', 'fsdp', 'ep'), None)
    in_specs = (tok_spec, P(None), P(None, None), P('ep', 'fsdp', None), P('ep', 'fsdp', None), P('ep', None, 'fsdp'), tok_spec)
    return jax.shard_map(local_block, mesh=mesh, in_specs=in_specs, out_specs=tok_spec, check_vma=False)
```

```python
import functools

import jax
import jax.numpy as jnp
from jax import lax
from jax.experimental import pallas as pl
from jax.experimental.pallas import tpu as pltpu
from jax.sharding import PartitionSpec as P

EPS = 1e-5
MESH = pl.DeviceIdType.MESH
HBM = pl.BlockSpec(memory_space=pl.ANY)
VMEM = pl.BlockSpec(memory_space=pltpu.VMEM)
F = 4
E = 4
CHUNKS = 8


O_SLOTS = 4
COLS = 8


def moe_kernel(hid, pos, gain, router, wg, wu, wd, back, hall, full, rows, logits,
               wbuf, xbuf, obuf, hbuf, acc_a, acc_b, pick, tok, out, squares,
               hy_s, hy_r, hs_s, hs_r, hf_s, hf_r, zr_s, zl_s, z_r, x_s, x_r,
               w_sem, x_sem, o_sem, r_sem, t_sem, g_sem, l_sem):
    half, z, j = lax.axis_index('dp'), lax.axis_index('fsdp'), lax.axis_index('ep')
    y, core = j // 2, j % 2
    sib = j + 1 - 2 * core
    across = (j + 2) % E
    experts, ff, width = wg.shape
    part = width // 2
    tokens, d_model = hid.shape
    capacity = hbuf.shape[0]
    pair = 2 * capacity
    chunk = tokens // CHUNKS
    cols = d_model // COLS
    early = tokens - chunk
    local = (wg, wu, wd)
    group = 3 * experts // 2
    steps = (F - 1) * group
    blocks = experts * E

    def region(p, f, h):
        return full.at[p % 3, p // 3, :, pl.ds(pl.multiple_of(f * width + h * part, 128), part)]

    def own(p):
        return local[p % 3].at[p // 3, :, pl.ds(pl.multiple_of(half * part, 128), part)]

    def along_z(p, f, src, step, sems):
        return pltpu.make_async_remote_copy(
            src_ref=src, dst_ref=region(p, f, half), send_sem=sems.at[p, f], recv_sem=z_r.at[p, f],
            device_id={'fsdp': z + step}, device_id_type=MESH)

    def along_x(p, f, h):
        return pltpu.make_async_remote_copy(
            src_ref=region(p, f, h), dst_ref=region(p, f, h), send_sem=x_s.at[p, f], recv_sem=x_r.at[p, f],
            device_id={'dp': 1 - half}, device_id_type=MESH)

    def own_start(lo, hi):
        for p in range(lo, hi):
            pl.when(z < F - 1)(lambda p=p: along_z(p, z, own(p), 1, zr_s).start())
            pl.when(z > 0)(lambda p=p: along_z(p, z, own(p), -1, zl_s).start())

    def arrive(p, d):
        def from_left():
            f = z - d
            along_z(p, f, region(p, f, half), 1, zr_s).wait_recv()
            pl.when(z < F - 1)(lambda: along_z(p, f, region(p, f, half), 1, zr_s).start())
            along_x(p, f, half).start()

        def from_right():
            f = z + d
            along_z(p, f, region(p, f, half), 1, zr_s).wait_recv()
            pl.when(z > 0)(lambda: along_z(p, f, region(p, f, half), -1, zl_s).start())
            along_x(p, f, half).start()

        pl.when(z >= d)(from_left)
        pl.when(z < F - d)(from_right)

    def arrivals(base, lo, hi):
        def body(i, c):
            arrive(base + i % group, i // group + 1)
            return c
        lax.fori_loop(lo, hi, body, 0)

    def each_piece(lo, hi, act):
        def body(i, c):
            p, f = lo + i // F, i % F
            act(p, f)
            return c
        lax.fori_loop(0, (hi - lo) * F, body, 0)

    def swapped(lo, hi):
        each_piece(lo, hi, lambda p, f: pl.when(z != f)(lambda: along_x(p, f, 1 - half).wait_recv()))

    def token_copy(src, owner, c, send, recv, target):
        return pltpu.make_async_remote_copy(
            src_ref=src, dst_ref=hall.at[owner, pl.ds(c * chunk, chunk)], send_sem=send.at[c], recv_sem=recv.at[c],
            device_id={'ep': target}, device_id_type=MESH)

    def mine(c):
        return hid.at[pl.ds(c * chunk, chunk)]

    def forward(lo, hi):
        for c in range(lo, hi):
            token_copy(mine(c), across, c, hy_s, hy_r, across).wait_recv()
            token_copy(hall.at[across, pl.ds(c * chunk, chunk)], across, c, hf_s, hf_r, sib).start()

    def device(ybit, cbit):
        return (y + ybit) % 2 * 2 + (core + cbit) % 2

    def token_load(r, n):
        owner = device(r // 4, r % 2)
        ns = pl.ds(pl.multiple_of(n * cols, 128), cols)
        near = pltpu.make_async_copy(hid.at[:, ns], tok.at[n % 2], t_sem.at[n % 2])
        far = pltpu.make_async_copy(hall.at[owner, :, ns], tok.at[n % 2], t_sem.at[n % 2])
        return near, far, r // 4 + r % 2 == 0

    def token_start(r, n):
        near, far, is_near = token_load(r, n)
        pl.when(is_near)(lambda: near.start())
        pl.when(jnp.logical_not(is_near))(lambda: far.start())

    def row_store(r, n):
        ns = pl.ds(pl.multiple_of(n * cols, 128), cols)
        dst = rows.at[r // 4 * 2 + r % 2, pl.ds(pl.multiple_of(r // 2 % 2 * pair, 16), pair), ns]
        return pltpu.make_async_copy(out.at[n % 2], dst, g_sem.at[n % 2])

    def mark_rows(r):
        owner = device(r // 4, r % 2)
        step = 32 if capacity % 32 == 0 else capacity

        def mark(i, c):
            e = i // (capacity // step)
            first = (i % (capacity // step)) * step
            want = pos[owner * experts + r // 2 % 2 * 2 + e]
            slot = first + lax.broadcasted_iota(jnp.int32, (step, tokens), 0)
            pick[pl.ds(pl.multiple_of(i * step, step), step), :] = jnp.where(slot == want, 1.0, 0.0).astype(jnp.bfloat16)
            return c
        lax.fori_loop(0, pair // step, mark, 0)

    def some_rows(act):
        step = min(tokens, 256)

        def body(i, c):
            act(pl.ds(pl.multiple_of(i * step, step), step))
            return c
        lax.fori_loop(0, tokens // step, body, 0)

    def route(r, n):
        ns = pl.ds(pl.multiple_of(n * cols, 128), cols)

        @pl.when(r == 0)
        def _():
            def add_squares(rs):
                x = tok[n % 2, rs, :].astype(jnp.float32)
                squares[rs, :] += jnp.sum(x * x, axis=-1, keepdims=True)
            some_rows(add_squares)

        @pl.when(r == 2)
        def _():
            def add_logits(rs):
                x = tok[n % 2, rs, :].astype(jnp.float32)
                scale = lax.rsqrt(squares[rs, :] / d_model + EPS)
                u = (x * scale * gain[:, ns]).astype(jnp.bfloat16)
                logits[rs, :] += lax.dot_general(
                    u, router[:, ns], (((1,), (1,)), ((), ())), preferred_element_type=jnp.float32)
            some_rows(add_logits)

    def pick_rows(r):
        token_start(r, 0)
        mark_rows(r)

        def column(n, c):
            token_load(r, n)[0].wait()
            pl.when(n + 1 < COLS)(lambda: token_start(r, n + 1))
            pl.when(n >= 2)(lambda: row_store(r, n - 2).wait())
            out[n % 2] = jnp.dot(pick[...], tok[n % 2], preferred_element_type=jnp.float32).astype(jnp.bfloat16)
            row_store(r, n).start()
            route(r, n)
            return c
        lax.fori_loop(0, COLS, column, 0)
        row_store(r, COLS - 2).wait()
        row_store(r, COLS - 1).wait()

    def pick_first_across():
        def load(n):
            ns = pl.ds(pl.multiple_of(n * cols, 128), cols)
            return pltpu.make_async_copy(
                hall.at[across, pl.ds(0, early), ns], tok.at[n % 2, pl.ds(0, early)], t_sem.at[n % 2])

        def load_last(n):
            return pltpu.make_async_copy(
                hall.at[across, pl.ds(early, chunk), pl.ds(n * cols, cols)], tok.at[0, pl.ds(n * chunk, chunk)], l_sem.at[n])

        mark_rows(4)
        forward(6, CHUNKS - 1)
        load(0).start()
        arrivals(group, 4, 5)

        def column(n, c):
            ns = pl.ds(pl.multiple_of(n * cols, 128), cols)
            load(n).wait()
            pl.when(n + 1 < COLS)(lambda: load(n + 1).start())
            got = jnp.dot(pick[:, :early], tok[n % 2, :early], preferred_element_type=jnp.float32).astype(jnp.bfloat16)
            xbuf[0, :, ns] = got[:capacity]
            xbuf[1, :, ns] = got[capacity:]
            return c
        lax.fori_loop(0, COLS, column, 0)
        forward(CHUNKS - 1, CHUNKS)
        for n in range(COLS):
            load_last(n).start()

        for n in range(COLS):
            load_last(n).wait()

        def column_last(n, c):
            ns = pl.ds(pl.multiple_of(n * cols, 128), cols)
            rest = tok[0, pl.ds(pl.multiple_of(n * chunk, 16), chunk), :]
            got = jnp.dot(pick[:, early:], rest, preferred_element_type=jnp.float32).astype(jnp.bfloat16)
            xbuf[0, :, ns] += got[:capacity]
            xbuf[1, :, ns] += got[capacity:]
            return c
        lax.fori_loop(0, COLS, column_last, 0)

    def weights(e, act):
        slot = e % 2
        for t in range(3):
            for f in range(F):
                fs = pl.ds(f * width, width)
                dst, sem = wbuf.at[slot, t, :, fs], w_sem.at[slot, t * F + f]
                pl.when(z == f)(lambda: act(pltpu.make_async_copy(local[t].at[e], dst, sem)))
                pl.when(z != f)(lambda: act(pltpu.make_async_copy(full.at[t, e, :, fs], dst, sem)))

    def start(copy):
        copy.start()

    def wait(copy):
        copy.wait()

    def place(k):
        m = k - 8
        e = jnp.where(k < 4, k // 2, jnp.where(k < 8, k % 2, 2 + m // 4))
        ybit = jnp.where(k < 4, 0, jnp.where(k < 8, 1, 1 - m % 2))
        cbit = jnp.where(k < 4, k % 2, jnp.where(k < 8, (k - 4) // 2, m % 4 // 2))
        return e, ybit, cbit

    def x_load(k):
        e, ybit, cbit = place(k)
        src = rows.at[ybit * 2 + cbit, pl.ds(pl.multiple_of(e * capacity, 16), capacity)]
        return pltpu.make_async_copy(src, xbuf.at[k % 2], x_sem.at[k % 2])

    def from_rows(k):
        return jnp.logical_or(k < 4, k > 5)

    def send(k):
        e, ybit, cbit = place(k)
        return pltpu.make_async_remote_copy(
            src_ref=obuf.at[k % O_SLOTS], dst_ref=back.at[j * experts + e], send_sem=o_sem.at[k % O_SLOTS],
            recv_sem=r_sem.at[j * experts + e], device_id={'ep': device(ybit, cbit)}, device_id_type=MESH)

    def keep(k):
        e, _, _ = place(k)
        return pltpu.make_async_copy(obuf.at[k % O_SLOTS], back.at[j * experts + e], o_sem.at[k % O_SLOTS])

    def is_local(k):
        _, ybit, cbit = place(k)
        return ybit + cbit == 0

    def sent(k):
        pl.when(is_local(k))(lambda: keep(k).wait())
        pl.when(jnp.logical_not(is_local(k)))(lambda: send(k).wait_send())

    def block(k, last):
        e, _, _ = place(k)
        slot, xs, os = e % 2, k % 2, k % O_SLOTS
        pl.when(k < 4)(lambda: arrivals(group, k, k + 1))
        for at, lo, hi in ((4, 5, 8), (5, 8, 9), (6, 9, 11), (7, 11, 13)):
            pl.when(k == at)(lambda: arrivals(group, lo, hi))

        @pl.when(k == 8)
        def _():
            arrivals(group, 13, steps)
            swapped(group, 2 * group)
            weights(2, start)
            weights(3, start)
            weights(2, wait)
        pl.when(k == 0)(lambda: weights(0, wait))
        pl.when(k == 2)(lambda: weights(1, wait))
        pl.when(k == 12)(lambda: weights(3, wait))

        pl.when(from_rows(k))(lambda: x_load(k).wait())
        pl.when(jnp.logical_and(from_rows(k), k + 1 < last))(lambda: x_load(k + 1).start())

        step = 16 if capacity % 16 == 0 else capacity
        def norm(r, c):
            rs = pl.ds(pl.multiple_of(r * step, step), step)
            x = xbuf[xs, rs, :].astype(jnp.float32)
            scale = lax.rsqrt(jnp.mean(x * x, axis=-1, keepdims=True) + EPS)
            xbuf[xs, rs, :] = (x * scale * gain[...]).astype(jnp.bfloat16)
            return c
        lax.fori_loop(0, capacity // step, norm, 0)

        acc_a[...] = jnp.zeros_like(acc_a)
        acc_b[...] = jnp.zeros_like(acc_b)
        def first(i, c):
            ks = pl.ds(pl.multiple_of(i * width, 128), width)
            u = xbuf[xs, :, ks]
            dims = (((1,), (1,)), ((), ()))
            acc_a[...] += lax.dot_general(u, wbuf[slot, 0, :, ks], dims, preferred_element_type=jnp.float32)
            acc_b[...] += lax.dot_general(u, wbuf[slot, 1, :, ks], dims, preferred_element_type=jnp.float32)
            return c
        lax.fori_loop(0, F, first, 0)
        a = acc_a[...]
        hbuf[...] = (a * jax.nn.sigmoid(a) * acc_b[...]).astype(jnp.bfloat16)

        pl.when(k >= O_SLOTS)(lambda: sent(k - O_SLOTS))
        def second(i, c):
            ns = pl.ds(pl.multiple_of(i * width, 128), width)
            obuf[os, :, ns] = jnp.dot(
                hbuf[...], wbuf[slot, 2, :, ns], preferred_element_type=jnp.float32).astype(jnp.bfloat16)
            return c
        lax.fori_loop(0, F, second, 0)
        pl.when(is_local(k))(lambda: keep(k).start())
        pl.when(jnp.logical_not(is_local(k)))(lambda: send(k).start())
        return last

    for c in range(CHUNKS):
        token_copy(mine(c), j, c, hs_s, hs_r, sib).start()
        token_copy(mine(c), j, c, hy_s, hy_r, across).start()
    own_start(0, group)
    squares[...] = jnp.zeros_like(squares)
    logits[...] = jnp.zeros_like(logits)

    def round_(r, c):
        @pl.when(r == 1)
        def _():
            for c in range(CHUNKS):
                token_copy(mine(c), sib, c, hs_s, hs_r, sib).wait_recv()

        @pl.when(r == 5)
        def _():
            for c in range(CHUNKS):
                token_copy(mine(c), sib, c, hf_s, hf_r, sib).wait_recv()

        pl.when(r == 4)(pick_first_across)
        pl.when(r != 4)(lambda: pick_rows(r))
        pl.when(r == 1)(lambda: arrivals(0, 0, 2))
        pl.when(r == 2)(lambda: arrivals(0, 2, 4))

        @pl.when(r == 3)
        def _():
            arrivals(0, 4, 6)
            forward(0, 2)
            arrivals(0, 6, 9)
            forward(2, 3)
            arrivals(0, 9, 12)
            forward(3, 4)
            own_start(group, 2 * group)
            arrivals(0, 12, 15)
            forward(4, 5)
            arrivals(0, 15, steps)
            forward(5, 6)
            swapped(0, group)
            weights(0, start)
            weights(1, start)

        def upto(r):
            return (jnp.where(r >= 3, 4, 0) + jnp.where(r >= 4, 2, 0) + jnp.where(r >= 5, 2, 0) + jnp.where(r >= 7, 8, 0))
        lo, hi = upto(r - 1), upto(r)
        pl.when(jnp.logical_and(lo < hi, r != 4))(lambda: x_load(lo).start())
        lax.fori_loop(lo, hi, lambda k, last: block(k, last), hi)
        return c

    lax.fori_loop(0, 8, round_, 0)

    for k in range(blocks - O_SLOTS, blocks):
        sent(jnp.int32(k))
    for c in range(CHUNKS):
        token_copy(mine(c), j, c, hy_s, hy_r, across).wait_send()
        token_copy(mine(c), j, c, hs_s, hs_r, sib).wait_send()
        token_copy(mine(c), j, c, hf_s, hf_r, sib).wait_send()

    def drain(p, f):
        src = region(p, f, half)
        pl.when(jnp.logical_and(z < F - 1, f <= z))(lambda: along_z(p, f, src, 1, zr_s).wait_send())
        pl.when(jnp.logical_and(z > 0, f >= z))(lambda: along_z(p, f, src, -1, zl_s).wait_send())
        pl.when(z != f)(lambda: along_x(p, f, half).wait_send())
    each_piece(0, 2 * group, drain)

    def arrived(n, c):
        def wait_block():
            pltpu.make_async_remote_copy(
                src_ref=obuf.at[0], dst_ref=back.at[n], send_sem=o_sem.at[0], recv_sem=r_sem.at[n],
                device_id={'ep': n // experts}, device_id_type=MESH).wait_recv()
        pl.when(n // experts != j)(wait_block)
        return c
    lax.fori_loop(0, blocks, arrived, 0)


def run_moe(hidden, positions, gain, router, w_gate, w_up, w_down, capacity):
    tokens, d_model = hidden.shape
    experts, ff, width = w_gate.shape
    bf16, f32, dma = jnp.bfloat16, jnp.float32, pltpu.SemaphoreType.DMA
    pieces = 3 * experts
    shapes = (
        (E * experts, capacity, d_model),
        (E, tokens, d_model),
        (3, experts, ff, d_model),
        (E, experts * capacity, d_model),
    )
    logits = jax.ShapeDtypeStruct((tokens, router.shape[0]), f32)
    results = pl.pallas_call(
        moe_kernel,
        out_shape=tuple(jax.ShapeDtypeStruct(shape, bf16) for shape in shapes) + (logits,),
        in_specs=[HBM, VMEM, VMEM, VMEM] + [HBM] * 3,
        out_specs=(HBM,) * 4 + (VMEM,),
        scratch_shapes=[
            pltpu.VMEM((2, 3, ff, d_model), bf16),
            pltpu.VMEM((2, capacity, d_model), bf16),
            pltpu.VMEM((O_SLOTS, capacity, d_model), bf16),
            pltpu.VMEM((capacity, ff), bf16),
            pltpu.VMEM((capacity, ff), f32),
            pltpu.VMEM((capacity, ff), f32),
            pltpu.VMEM((2 * capacity, tokens), bf16),
            pltpu.VMEM((2, tokens, d_model // COLS), bf16),
            pltpu.VMEM((2, 2 * capacity, d_model // COLS), bf16),
            pltpu.VMEM((tokens, 1), f32),
        ] + [dma((CHUNKS,)) for _ in range(6)] + [dma((pieces, F)) for _ in range(5)] + [
            dma((2, 3 * F)), dma((2,)), dma((O_SLOTS,)), dma((E * experts,)), dma((2,)), dma((2,)), dma((COLS,)),
        ],
        compiler_params=pltpu.CompilerParams(has_side_effects=True, vmem_limit_bytes=63 * 1024 * 1024),
        name='moe',
    )(hidden, positions, gain, router, w_gate, w_up, w_down)
    return results[0], results[-1]


TILE = 128
SPAN = 16
WINDOWS = 32


def combine_kernel(starts, lists, logits, hid, back, out, buf, base, count, acc, sem):
    i = pl.program_id(0)
    num_experts = starts.shape[0] // (pl.num_programs(0) + 1)
    capacity = back.shape[0] // num_experts
    d_model = back.shape[1]
    cols = d_model // 4

    def window(row, s, n):
        src = back.at[pl.ds(pl.multiple_of(row, SPAN), SPAN)]
        return pltpu.make_async_copy(src, buf.at[s, pl.ds(pl.multiple_of(n * SPAN, SPAN), SPAN)], sem.at[s])

    def fill(tile, turn, s):
        first = turn * WINDOWS

        def clear(n, c):
            base[s, n] = -100000
            return c
        lax.fori_loop(0, WINDOWS, clear, 0)

        def expert(e, n):
            lo, hi = starts[tile * num_experts + e], starts[(tile + 1) * num_experts + e]

            def one(c, n):
                @pl.when(jnp.logical_and(n >= first, n < first + WINDOWS))
                def _():
                    row = e * capacity + c * SPAN
                    base[s, n - first] = row
                    window(row, s, n - first).start()
                return n + 1
            return lax.fori_loop(lo // SPAN, jnp.where(hi > lo, (hi + SPAN - 1) // SPAN, lo // SPAN), one, n)
        count[s] = lax.fori_loop(0, num_experts, expert, jnp.int32(0))

    by_token = lists[...].T
    slots = [by_token[:, k:k + 1] for k in range(2)]
    expert_ids = lax.broadcasted_iota(jnp.int32, logits.shape, 1)
    r0, r1 = [
        jnp.sum(jnp.where(by_token[:, 2 + k:3 + k] == expert_ids, logits[...], 0.0), axis=1, keepdims=True) for k in range(2)]
    top = jnp.maximum(r0, r1)
    e0, e1 = jnp.exp(r0 - top), jnp.exp(r1 - top)
    p0, p1 = e0 / (e0 + e1), e1 / (e0 + e1)

    def use(turn, s):
        def arrived(n, c):
            window(0, s, 0).wait()
            return c
        lax.fori_loop(0, jnp.minimum(count[s] - turn * WINDOWS, WINDOWS), arrived, 0)
        lane = lax.broadcasted_iota(jnp.int32, (1, WINDOWS * SPAN), 1)
        row = jnp.zeros_like(lane)
        for n in range(WINDOWS):
            row = jnp.where(lane // SPAN == n, base[s, n], row)
        row = row + lane % SPAN
        pick = jnp.concatenate([jnp.where(slot == row, 1.0, 0.0) for slot in slots], axis=0).astype(jnp.bfloat16)

        def column(n, c):
            ns = pl.ds(pl.multiple_of(n * cols, 128), cols)
            got = jnp.dot(pick, buf[s, :, ns], preferred_element_type=jnp.float32)
            acc[:, ns] += p0 * got[:TILE] + p1 * got[TILE:]
            return c
        lax.fori_loop(0, 4, column, 0)

    s = i % 2

    @pl.when(i == 0)
    def _():
        buf[...] = jnp.zeros_like(buf)
        fill(i, 0, s)
    pl.when(i + 1 < pl.num_programs(0))(lambda: fill(i + 1, 0, 1 - s))
    acc[...] = hid[...].astype(jnp.float32)
    use(0, s)

    def more(turn, c):
        fill(i, turn, s)
        use(turn, s)
        return c
    lax.fori_loop(1, (count[s] + WINDOWS - 1) // WINDOWS, more, 0)
    out[...] = acc[...].astype(out.dtype)


def combine(hidden, back, starts, lists, logits):
    tokens, d_model = hidden.shape
    tiles = tokens // TILE
    row = pl.BlockSpec((TILE, d_model), lambda i: (i, 0))

    return pl.pallas_call(
        combine_kernel,
        grid=(tiles,),
        out_shape=jax.ShapeDtypeStruct(hidden.shape, hidden.dtype),
        in_specs=[
            pl.BlockSpec(memory_space=pltpu.SMEM),
            pl.BlockSpec((lists.shape[0], TILE), lambda i: (0, i)),
            pl.BlockSpec((TILE, logits.shape[1]), lambda i: (i, 0)),
            row,
            HBM,
        ],
        out_specs=row,
        scratch_shapes=[
            pltpu.VMEM((2, WINDOWS * SPAN, d_model), jnp.bfloat16),
            pltpu.SMEM((2, WINDOWS), jnp.int32),
            pltpu.SMEM((2,), jnp.int32),
            pltpu.VMEM((TILE, d_model), jnp.float32),
            pltpu.SemaphoreType.DMA((2,)),
        ],
        compiler_params=pltpu.CompilerParams(dimension_semantics=('arbitrary',)),
        name='combine',
    )(starts.reshape(-1), lists, logits, hidden, back)


def local_block(hidden, norm_gain, w_router, w_gate, w_up, w_down, top2_ids):
    tok_local, d_model = hidden.shape
    num_experts = w_router.shape[1]
    capacity = (5 * tok_local + 2 * num_experts - 1) // (2 * num_experts)
    experts = num_experts // E

    ids = [top2_ids[:, k][None, :] for k in range(2)]
    expert_ids = jnp.arange(num_experts, dtype=jnp.int32)[:, None]
    chosen = jnp.logical_or(ids[0] == expert_ids, ids[1] == expert_ids)
    before = jnp.cumsum(chosen.astype(jnp.int32), axis=1) - 1
    positions = jnp.where(chosen, before, -1)
    place = [jnp.sum(jnp.where(ids[k] == expert_ids, before, 0), axis=0) for k in range(2)]
    positions = lax.all_to_all(positions.reshape(E, experts, tok_local), 'ep', 0, 0)
    positions = positions.reshape(E * experts, 1, tok_local)

    gain = norm_gain.astype(jnp.float32).reshape(1, d_model)
    back, logits = run_moe(hidden, positions, gain, w_router.T, jnp.swapaxes(w_gate, 1, 2), jnp.swapaxes(w_up, 1, 2), w_down, capacity)
    back = back.reshape(num_experts * capacity, d_model)

    rows = [jnp.where(place[k] < capacity, top2_ids[:, k] * capacity + place[k], -1) for k in range(2)]
    lists = jnp.stack(rows + [top2_ids[:, 0], top2_ids[:, 1]] + [jnp.zeros_like(place[0])] * 4)
    counts = jnp.minimum(before[:, TILE - 1::TILE].T + 1, capacity)
    starts = jnp.concatenate([jnp.zeros((1, num_experts), jnp.int32), counts], axis=0)
    return combine(hidden, back, starts, lists, logits)


def solution(mesh):
    tok_spec = P(('dp', 'fsdp', 'ep'), None)
    in_specs = (tok_spec, P(None), P(None, None), P('ep', 'fsdp', None), P('ep', 'fsdp', None), P('ep', None, 'fsdp'), tok_spec)
    return jax.shard_map(local_block, mesh=mesh, in_specs=in_specs, out_specs=tok_spec, check_vma=False)
```

```python
import functools

import jax
import jax.numpy as jnp
from jax import lax
from jax.experimental import pallas as pl
from jax.experimental.pallas import tpu as pltpu
from jax.sharding import PartitionSpec as P

EPS = 1e-5
MESH = pl.DeviceIdType.MESH
HBM = pl.BlockSpec(memory_space=pl.ANY)
VMEM = pl.BlockSpec(memory_space=pltpu.VMEM)
F = 4
E = 4
CHUNKS = 8


O_SLOTS = 4
COLS = 8


def moe_kernel(hid, pos, gain, router, wg, wu, wd, back, hall, full, rows, logits,
               wbuf, xbuf, obuf, hbuf, acc_a, acc_b, pick, tok, out, squares,
               hy_s, hy_r, hs_s, hs_r, hf_s, hf_r, zr_s, zl_s, z_r, x_s, x_r,
               w_sem, x_sem, o_sem, r_sem, t_sem, g_sem, l_sem):
    half, z, j = lax.axis_index('dp'), lax.axis_index('fsdp'), lax.axis_index('ep')
    y, core = j // 2, j % 2
    sib = j + 1 - 2 * core
    across = (j + 2) % E
    experts, ff, width = wg.shape
    part = width // 2
    tokens, d_model = hid.shape
    capacity = hbuf.shape[0]
    pair = 2 * capacity
    chunk = tokens // CHUNKS
    cols = d_model // COLS
    early = tokens - chunk
    local = (wg, wu, wd)
    group = 3 * experts // 2
    steps = (F - 1) * group
    blocks = experts * E

    def region(p, f, h):
        return full.at[p % 3, p // 3, :, pl.ds(pl.multiple_of(f * width + h * part, 128), part)]

    def own(p):
        return local[p % 3].at[p // 3, :, pl.ds(pl.multiple_of(half * part, 128), part)]

    def along_z(p, f, src, step, sems):
        return pltpu.make_async_remote_copy(
            src_ref=src, dst_ref=region(p, f, half), send_sem=sems.at[p, f], recv_sem=z_r.at[p, f],
            device_id={'fsdp': z + step}, device_id_type=MESH)

    def along_x(p, f, h):
        return pltpu.make_async_remote_copy(
            src_ref=region(p, f, h), dst_ref=region(p, f, h), send_sem=x_s.at[p, f], recv_sem=x_r.at[p, f],
            device_id={'dp': 1 - half}, device_id_type=MESH)

    def own_start(lo, hi):
        for p in range(lo, hi):
            pl.when(z < F - 1)(lambda p=p: along_z(p, z, own(p), 1, zr_s).start())
            pl.when(z > 0)(lambda p=p: along_z(p, z, own(p), -1, zl_s).start())

    def arrive(p, d):
        def from_left():
            f = z - d
            along_z(p, f, region(p, f, half), 1, zr_s).wait_recv()
            pl.when(z < F - 1)(lambda: along_z(p, f, region(p, f, half), 1, zr_s).start())
            along_x(p, f, half).start()

        def from_right():
            f = z + d
            along_z(p, f, region(p, f, half), 1, zr_s).wait_recv()
            pl.when(z > 0)(lambda: along_z(p, f, region(p, f, half), -1, zl_s).start())
            along_x(p, f, half).start()

        pl.when(z >= d)(from_left)
        pl.when(z < F - d)(from_right)

    def arrivals(base, lo, hi):
        def body(i, c):
            arrive(base + i % group, i // group + 1)
            return c
        lax.fori_loop(lo, hi, body, 0)

    def each_piece(lo, hi, act):
        def body(i, c):
            p, f = lo + i // F, i % F
            act(p, f)
            return c
        lax.fori_loop(0, (hi - lo) * F, body, 0)

    def swapped(lo, hi):
        each_piece(lo, hi, lambda p, f: pl.when(z != f)(lambda: along_x(p, f, 1 - half).wait_recv()))

    def token_copy(src, owner, c, send, recv, target):
        return pltpu.make_async_remote_copy(
            src_ref=src, dst_ref=hall.at[owner, pl.ds(c * chunk, chunk)], send_sem=send.at[c], recv_sem=recv.at[c],
            device_id={'ep': target}, device_id_type=MESH)

    def mine(c):
        return hid.at[pl.ds(c * chunk, chunk)]

    def forward(lo, hi):
        for c in range(lo, hi):
            token_copy(mine(c), across, c, hy_s, hy_r, across).wait_recv()
            token_copy(hall.at[across, pl.ds(c * chunk, chunk)], across, c, hf_s, hf_r, sib).start()

    def device(ybit, cbit):
        return (y + ybit) % 2 * 2 + (core + cbit) % 2

    def token_load(r, n):
        owner = device(r // 4, r % 2)
        ns = pl.ds(pl.multiple_of(n * cols, 128), cols)
        near = pltpu.make_async_copy(hid.at[:, ns], tok.at[n % 2], t_sem.at[n % 2])
        far = pltpu.make_async_copy(hall.at[owner, :, ns], tok.at[n % 2], t_sem.at[n % 2])
        return near, far, r // 4 + r % 2 == 0

    def token_start(r, n):
        near, far, is_near = token_load(r, n)
        pl.when(is_near)(lambda: near.start())
        pl.when(jnp.logical_not(is_near))(lambda: far.start())

    def row_store(r, n):
        ns = pl.ds(pl.multiple_of(n * cols, 128), cols)
        dst = rows.at[r // 4 * 2 + r % 2, pl.ds(pl.multiple_of(r // 2 % 2 * pair, 16), pair), ns]
        return pltpu.make_async_copy(out.at[n % 2], dst, g_sem.at[n % 2])

    def mark_rows(r):
        owner = device(r // 4, r % 2)
        step = 32 if capacity % 32 == 0 else capacity

        def mark(i, c):
            e = i // (capacity // step)
            first = (i % (capacity // step)) * step
            want = pos[owner * experts + r // 2 % 2 * 2 + e]
            slot = first + lax.broadcasted_iota(jnp.int32, (step, tokens), 0)
            pick[pl.ds(pl.multiple_of(i * step, step), step), :] = jnp.where(slot == want, 1.0, 0.0).astype(jnp.bfloat16)
            return c
        lax.fori_loop(0, pair // step, mark, 0)

    def some_rows(act):
        step = min(tokens, 256)

        def body(i, c):
            act(pl.ds(pl.multiple_of(i * step, step), step))
            return c
        lax.fori_loop(0, tokens // step, body, 0)

    def route(r, n):
        ns = pl.ds(pl.multiple_of(n * cols, 128), cols)

        @pl.when(r == 0)
        def _():
            def add_squares(rs):
                x = tok[n % 2, rs, :].astype(jnp.float32)
                squares[rs, :] += jnp.sum(x * x, axis=-1, keepdims=True)
            some_rows(add_squares)

        @pl.when(r == 2)
        def _():
            def add_logits(rs):
                x = tok[n % 2, rs, :].astype(jnp.float32)
                scale = lax.rsqrt(squares[rs, :] / d_model + EPS)
                u = (x * scale * gain[:, ns]).astype(jnp.bfloat16)
                logits[rs, :] += lax.dot_general(
                    u, router[:, ns], (((1,), (1,)), ((), ())), preferred_element_type=jnp.float32)
            some_rows(add_logits)

    def pick_rows(r):
        token_start(r, 0)
        mark_rows(r)

        def column(n, c):
            token_load(r, n)[0].wait()
            pl.when(n + 1 < COLS)(lambda: token_start(r, n + 1))
            pl.when(n >= 2)(lambda: row_store(r, n - 2).wait())
            out[n % 2] = jnp.dot(pick[...], tok[n % 2], preferred_element_type=jnp.float32).astype(jnp.bfloat16)
            row_store(r, n).start()
            route(r, n)
            return c
        lax.fori_loop(0, COLS, column, 0)
        row_store(r, COLS - 2).wait()
        row_store(r, COLS - 1).wait()

    def pick_first_across():
        def load(n):
            ns = pl.ds(pl.multiple_of(n * cols, 128), cols)
            return pltpu.make_async_copy(
                hall.at[across, pl.ds(0, early), ns], tok.at[n % 2, pl.ds(0, early)], t_sem.at[n % 2])

        def load_last(n):
            return pltpu.make_async_copy(
                hall.at[across, pl.ds(early, chunk), pl.ds(n * cols, cols)], tok.at[0, pl.ds(n * chunk, chunk)], l_sem.at[n])

        mark_rows(4)
        forward(6, CHUNKS - 1)
        load(0).start()
        arrivals(group, 4, 5)

        def column(n, c):
            ns = pl.ds(pl.multiple_of(n * cols, 128), cols)
            load(n).wait()
            pl.when(n + 1 < COLS)(lambda: load(n + 1).start())
            got = jnp.dot(pick[:, :early], tok[n % 2, :early], preferred_element_type=jnp.float32).astype(jnp.bfloat16)
            xbuf[0, :, ns] = got[:capacity]
            xbuf[1, :, ns] = got[capacity:]
            return c
        lax.fori_loop(0, COLS, column, 0)
        forward(CHUNKS - 1, CHUNKS)
        for n in range(COLS):
            load_last(n).start()

        for n in range(COLS):
            load_last(n).wait()

        def column_last(n, c):
            ns = pl.ds(pl.multiple_of(n * cols, 128), cols)
            rest = tok[0, pl.ds(pl.multiple_of(n * chunk, 16), chunk), :]
            got = jnp.dot(pick[:, early:], rest, preferred_element_type=jnp.float32).astype(jnp.bfloat16)
            xbuf[0, :, ns] += got[:capacity]
            xbuf[1, :, ns] += got[capacity:]
            return c
        lax.fori_loop(0, COLS, column_last, 0)

    def weights(e, act):
        slot = e % 2
        for t in range(3):
            for f in range(F):
                fs = pl.ds(f * width, width)
                dst, sem = wbuf.at[slot, t, :, fs], w_sem.at[slot, t * F + f]
                pl.when(z == f)(lambda: act(pltpu.make_async_copy(local[t].at[e], dst, sem)))
                pl.when(z != f)(lambda: act(pltpu.make_async_copy(full.at[t, e, :, fs], dst, sem)))

    def start(copy):
        copy.start()

    def wait(copy):
        copy.wait()

    def place(k):
        m = k - 8
        e = jnp.where(k < 4, k // 2, jnp.where(k < 8, k % 2, 2 + m // 4))
        ybit = jnp.where(k < 4, 0, jnp.where(k < 8, 1, 1 - m % 2))
        cbit = jnp.where(k < 4, k % 2, jnp.where(k < 8, (k - 4) // 2, m % 4 // 2))
        return e, ybit, cbit

    def x_load(k):
        e, ybit, cbit = place(k)
        src = rows.at[ybit * 2 + cbit, pl.ds(pl.multiple_of(e * capacity, 16), capacity)]
        return pltpu.make_async_copy(src, xbuf.at[k % 2], x_sem.at[k % 2])

    def from_rows(k):
        return jnp.logical_or(k < 4, k > 5)

    def send(k):
        e, ybit, cbit = place(k)
        return pltpu.make_async_remote_copy(
            src_ref=obuf.at[k % O_SLOTS], dst_ref=back.at[j * experts + e], send_sem=o_sem.at[k % O_SLOTS],
            recv_sem=r_sem.at[j * experts + e], device_id={'ep': device(ybit, cbit)}, device_id_type=MESH)

    def keep(k):
        e, _, _ = place(k)
        return pltpu.make_async_copy(obuf.at[k % O_SLOTS], back.at[j * experts + e], o_sem.at[k % O_SLOTS])

    def is_local(k):
        _, ybit, cbit = place(k)
        return ybit + cbit == 0

    def sent(k):
        pl.when(is_local(k))(lambda: keep(k).wait())
        pl.when(jnp.logical_not(is_local(k)))(lambda: send(k).wait_send())

    def block(k, last):
        e, _, _ = place(k)
        slot, xs, os = e % 2, k % 2, k % O_SLOTS
        pl.when(k < 4)(lambda: arrivals(group, k, k + 1))
        for at, lo, hi in ((4, 5, 8), (5, 8, 9), (6, 9, 11), (7, 11, 13)):
            pl.when(k == at)(lambda: arrivals(group, lo, hi))

        @pl.when(k == 8)
        def _():
            arrivals(group, 13, steps - 3)
            swapped(group, group + 3)
            weights(2, start)
            weights(2, wait)
        pl.when(k == 9)(lambda: arrivals(group, steps - 3, steps))

        @pl.when(k == 10)
        def _():
            swapped(group + 3, 2 * group)
            weights(3, start)
        pl.when(k == 0)(lambda: weights(0, wait))
        pl.when(k == 2)(lambda: weights(1, wait))
        pl.when(k == 12)(lambda: weights(3, wait))

        pl.when(from_rows(k))(lambda: x_load(k).wait())
        pl.when(jnp.logical_and(from_rows(k), k + 1 < last))(lambda: x_load(k + 1).start())

        step = 16 if capacity % 16 == 0 else capacity
        def norm(r, c):
            rs = pl.ds(pl.multiple_of(r * step, step), step)
            x = xbuf[xs, rs, :].astype(jnp.float32)
            scale = lax.rsqrt(jnp.mean(x * x, axis=-1, keepdims=True) + EPS)
            xbuf[xs, rs, :] = (x * scale * gain[...]).astype(jnp.bfloat16)
            return c
        lax.fori_loop(0, capacity // step, norm, 0)

        acc_a[...] = jnp.zeros_like(acc_a)
        acc_b[...] = jnp.zeros_like(acc_b)
        def first(i, c):
            ks = pl.ds(pl.multiple_of(i * width, 128), width)
            u = xbuf[xs, :, ks]
            dims = (((1,), (1,)), ((), ()))
            acc_a[...] += lax.dot_general(u, wbuf[slot, 0, :, ks], dims, preferred_element_type=jnp.float32)
            acc_b[...] += lax.dot_general(u, wbuf[slot, 1, :, ks], dims, preferred_element_type=jnp.float32)
            return c
        lax.fori_loop(0, F, first, 0)
        a = acc_a[...]
        hbuf[...] = (a * jax.nn.sigmoid(a) * acc_b[...]).astype(jnp.bfloat16)

        pl.when(k >= O_SLOTS)(lambda: sent(k - O_SLOTS))
        def second(i, c):
            ns = pl.ds(pl.multiple_of(i * width, 128), width)
            obuf[os, :, ns] = jnp.dot(
                hbuf[...], wbuf[slot, 2, :, ns], preferred_element_type=jnp.float32).astype(jnp.bfloat16)
            return c
        lax.fori_loop(0, F, second, 0)
        pl.when(is_local(k))(lambda: keep(k).start())
        pl.when(jnp.logical_not(is_local(k)))(lambda: send(k).start())
        return last

    for c in range(CHUNKS):
        token_copy(mine(c), j, c, hs_s, hs_r, sib).start()
        token_copy(mine(c), j, c, hy_s, hy_r, across).start()
    own_start(0, group)
    squares[...] = jnp.zeros_like(squares)
    logits[...] = jnp.zeros_like(logits)

    def round_(r, c):
        @pl.when(r == 1)
        def _():
            for c in range(CHUNKS):
                token_copy(mine(c), sib, c, hs_s, hs_r, sib).wait_recv()

        @pl.when(r == 5)
        def _():
            for c in range(CHUNKS):
                token_copy(mine(c), sib, c, hf_s, hf_r, sib).wait_recv()

        pl.when(r == 4)(pick_first_across)
        pl.when(r != 4)(lambda: pick_rows(r))
        pl.when(r == 0)(lambda: arrivals(0, 0, 1))
        pl.when(r == 1)(lambda: arrivals(0, 1, 2))
        pl.when(r == 2)(lambda: arrivals(0, 2, 4))

        @pl.when(r == 3)
        def _():
            arrivals(0, 4, 6)
            forward(0, 2)
            arrivals(0, 6, 9)
            forward(2, 3)
            arrivals(0, 9, 12)
            forward(3, 4)
            own_start(group, 2 * group)
            arrivals(0, 12, 15)
            forward(4, 5)
            arrivals(0, 15, steps)
            forward(5, 6)
            swapped(0, group)
            weights(0, start)
            weights(1, start)

        def upto(r):
            return (jnp.where(r >= 3, 4, 0) + jnp.where(r >= 4, 2, 0) + jnp.where(r >= 5, 2, 0) + jnp.where(r >= 7, 8, 0))
        lo, hi = upto(r - 1), upto(r)
        pl.when(jnp.logical_and(lo < hi, r != 4))(lambda: x_load(lo).start())
        lax.fori_loop(lo, hi, lambda k, last: block(k, last), hi)
        return c

    lax.fori_loop(0, 8, round_, 0)

    for k in range(blocks - O_SLOTS, blocks):
        sent(jnp.int32(k))
    for c in range(CHUNKS):
        token_copy(mine(c), j, c, hy_s, hy_r, across).wait_send()
        token_copy(mine(c), j, c, hs_s, hs_r, sib).wait_send()
        token_copy(mine(c), j, c, hf_s, hf_r, sib).wait_send()

    def drain(p, f):
        src = region(p, f, half)
        pl.when(jnp.logical_and(z < F - 1, f <= z))(lambda: along_z(p, f, src, 1, zr_s).wait_send())
        pl.when(jnp.logical_and(z > 0, f >= z))(lambda: along_z(p, f, src, -1, zl_s).wait_send())
        pl.when(z != f)(lambda: along_x(p, f, half).wait_send())
    each_piece(0, 2 * group, drain)

    def arrived(n, c):
        def wait_block():
            pltpu.make_async_remote_copy(
                src_ref=obuf.at[0], dst_ref=back.at[n], send_sem=o_sem.at[0], recv_sem=r_sem.at[n],
                device_id={'ep': n // experts}, device_id_type=MESH).wait_recv()
        pl.when(n // experts != j)(wait_block)
        return c
    lax.fori_loop(0, blocks, arrived, 0)


def run_moe(hidden, positions, gain, router, w_gate, w_up, w_down, capacity):
    tokens, d_model = hidden.shape
    experts, ff, width = w_gate.shape
    bf16, f32, dma = jnp.bfloat16, jnp.float32, pltpu.SemaphoreType.DMA
    pieces = 3 * experts
    shapes = (
        (E * experts, capacity, d_model),
        (E, tokens, d_model),
        (3, experts, ff, d_model),
        (E, experts * capacity, d_model),
    )
    logits = jax.ShapeDtypeStruct((tokens, router.shape[0]), f32)
    results = pl.pallas_call(
        moe_kernel,
        out_shape=tuple(jax.ShapeDtypeStruct(shape, bf16) for shape in shapes) + (logits,),
        in_specs=[HBM, VMEM, VMEM, VMEM] + [HBM] * 3,
        out_specs=(HBM,) * 4 + (VMEM,),
        scratch_shapes=[
            pltpu.VMEM((2, 3, ff, d_model), bf16),
            pltpu.VMEM((2, capacity, d_model), bf16),
            pltpu.VMEM((O_SLOTS, capacity, d_model), bf16),
            pltpu.VMEM((capacity, ff), bf16),
            pltpu.VMEM((capacity, ff), f32),
            pltpu.VMEM((capacity, ff), f32),
            pltpu.VMEM((2 * capacity, tokens), bf16),
            pltpu.VMEM((2, tokens, d_model // COLS), bf16),
            pltpu.VMEM((2, 2 * capacity, d_model // COLS), bf16),
            pltpu.VMEM((tokens, 1), f32),
        ] + [dma((CHUNKS,)) for _ in range(6)] + [dma((pieces, F)) for _ in range(5)] + [
            dma((2, 3 * F)), dma((2,)), dma((O_SLOTS,)), dma((E * experts,)), dma((2,)), dma((2,)), dma((COLS,)),
        ],
        compiler_params=pltpu.CompilerParams(has_side_effects=True, vmem_limit_bytes=63 * 1024 * 1024),
        name='moe',
    )(hidden, positions, gain, router, w_gate, w_up, w_down)
    return results[0], results[-1]


TILE = 128
SPAN = 16
WINDOWS = 40


def combine_kernel(starts, lists, logits, hid, back, out, buf, base, count, acc, sem):
    i = pl.program_id(0)
    num_experts = starts.shape[0] // (pl.num_programs(0) + 1)
    capacity = back.shape[0] // num_experts
    d_model = back.shape[1]
    cols = d_model // 4

    def window(row, s, n):
        src = back.at[pl.ds(pl.multiple_of(row, SPAN), SPAN)]
        return pltpu.make_async_copy(src, buf.at[s, pl.ds(pl.multiple_of(n * SPAN, SPAN), SPAN)], sem.at[s])

    def fill(tile, turn, s):
        first = turn * WINDOWS

        def clear(n, c):
            base[s, n] = -100000
            return c
        lax.fori_loop(0, WINDOWS, clear, 0)

        def expert(e, n):
            lo, hi = starts[tile * num_experts + e], starts[(tile + 1) * num_experts + e]

            def one(c, n):
                @pl.when(jnp.logical_and(n >= first, n < first + WINDOWS))
                def _():
                    row = e * capacity + c * SPAN
                    base[s, n - first] = row
                    window(row, s, n - first).start()
                return n + 1
            return lax.fori_loop(lo // SPAN, jnp.where(hi > lo, (hi + SPAN - 1) // SPAN, lo // SPAN), one, n)
        count[s] = lax.fori_loop(0, num_experts, expert, jnp.int32(0))

    by_token = lists[...].T
    slots = [by_token[:, k:k + 1] for k in range(2)]
    expert_ids = lax.broadcasted_iota(jnp.int32, logits.shape, 1)
    r0, r1 = [
        jnp.sum(jnp.where(by_token[:, 2 + k:3 + k] == expert_ids, logits[...], 0.0), axis=1, keepdims=True) for k in range(2)]
    top = jnp.maximum(r0, r1)
    e0, e1 = jnp.exp(r0 - top), jnp.exp(r1 - top)
    p0, p1 = e0 / (e0 + e1), e1 / (e0 + e1)

    def use(turn, s):
        def arrived(n, c):
            window(0, s, 0).wait()
            return c
        lax.fori_loop(0, jnp.minimum(count[s] - turn * WINDOWS, WINDOWS), arrived, 0)
        lane = lax.broadcasted_iota(jnp.int32, (1, WINDOWS * SPAN), 1)
        row = jnp.zeros_like(lane)
        for n in range(WINDOWS):
            row = jnp.where(lane // SPAN == n, base[s, n], row)
        row = row + lane % SPAN
        pick = jnp.concatenate([jnp.where(slot == row, 1.0, 0.0) for slot in slots], axis=0).astype(jnp.bfloat16)

        def column(n, c):
            ns = pl.ds(pl.multiple_of(n * cols, 128), cols)
            got = jnp.dot(pick, buf[s, :, ns], preferred_element_type=jnp.float32)
            acc[:, ns] += p0 * got[:TILE] + p1 * got[TILE:]
            return c
        lax.fori_loop(0, 4, column, 0)

    s = i % 2

    @pl.when(i == 0)
    def _():
        buf[...] = jnp.zeros_like(buf)
        fill(i, 0, s)
    pl.when(i + 1 < pl.num_programs(0))(lambda: fill(i + 1, 0, 1 - s))
    acc[...] = hid[...].astype(jnp.float32)
    use(0, s)

    def more(turn, c):
        fill(i, turn, s)
        use(turn, s)
        return c
    lax.fori_loop(1, (count[s] + WINDOWS - 1) // WINDOWS, more, 0)
    out[...] = acc[...].astype(out.dtype)


def combine(hidden, back, starts, lists, logits):
    tokens, d_model = hidden.shape
    tiles = tokens // TILE
    row = pl.BlockSpec((TILE, d_model), lambda i: (i, 0))

    return pl.pallas_call(
        combine_kernel,
        grid=(tiles,),
        out_shape=jax.ShapeDtypeStruct(hidden.shape, hidden.dtype),
        in_specs=[
            pl.BlockSpec(memory_space=pltpu.SMEM),
            pl.BlockSpec((lists.shape[0], TILE), lambda i: (0, i)),
            pl.BlockSpec((TILE, logits.shape[1]), lambda i: (i, 0)),
            row,
            HBM,
        ],
        out_specs=row,
        scratch_shapes=[
            pltpu.VMEM((2, WINDOWS * SPAN, d_model), jnp.bfloat16),
            pltpu.SMEM((2, WINDOWS), jnp.int32),
            pltpu.SMEM((2,), jnp.int32),
            pltpu.VMEM((TILE, d_model), jnp.float32),
            pltpu.SemaphoreType.DMA((2,)),
        ],
        compiler_params=pltpu.CompilerParams(dimension_semantics=('arbitrary',)),
        name='combine',
    )(starts.reshape(-1), lists, logits, hidden, back)


def local_block(hidden, norm_gain, w_router, w_gate, w_up, w_down, top2_ids):
    tok_local, d_model = hidden.shape
    num_experts = w_router.shape[1]
    capacity = (5 * tok_local + 2 * num_experts - 1) // (2 * num_experts)
    experts = num_experts // E

    ids = [top2_ids[:, k][None, :] for k in range(2)]
    expert_ids = jnp.arange(num_experts, dtype=jnp.int32)[:, None]
    chosen = jnp.logical_or(ids[0] == expert_ids, ids[1] == expert_ids)
    before = jnp.cumsum(chosen.astype(jnp.int32), axis=1) - 1
    positions = jnp.where(chosen, before, -1)
    place = [jnp.sum(jnp.where(ids[k] == expert_ids, before, 0), axis=0) for k in range(2)]
    positions = lax.all_to_all(positions.reshape(E, experts, tok_local), 'ep', 0, 0)
    positions = positions.reshape(E * experts, 1, tok_local)

    gain = norm_gain.astype(jnp.float32).reshape(1, d_model)
    back, logits = run_moe(hidden, positions, gain, w_router.T, jnp.swapaxes(w_gate, 1, 2), jnp.swapaxes(w_up, 1, 2), w_down, capacity)
    back = back.reshape(num_experts * capacity, d_model)

    rows = [jnp.where(place[k] < capacity, top2_ids[:, k] * capacity + place[k], -1) for k in range(2)]
    lists = jnp.stack(rows + [top2_ids[:, 0], top2_ids[:, 1]] + [jnp.zeros_like(place[0])] * 4)
    counts = jnp.minimum(before[:, TILE - 1::TILE].T + 1, capacity)
    starts = jnp.concatenate([jnp.zeros((1, num_experts), jnp.int32), counts], axis=0)
    return combine(hidden, back, starts, lists, logits)


def solution(mesh):
    tok_spec = P(('dp', 'fsdp', 'ep'), None)
    in_specs = (tok_spec, P(None), P(None, None), P('ep', 'fsdp', None), P('ep', 'fsdp', None), P('ep', None, 'fsdp'), tok_spec)
    return jax.shard_map(local_block, mesh=mesh, in_specs=in_specs, out_specs=tok_spec, check_vma=False)
```
